128 devices in a mesh: tasks: 1, cols: 2 (over core), rows: 64 (over z, y, x).
Axes of the slice: x: 4, y: 4, z: 4, core: 2. Of those that a mesh axis runs over, the one named last changes fastest.
Arguments:
- points: bfloat16 [131072, 128], P(('tasks', 'rows', 'cols'))
- rhs_vecs: bfloat16 [131072, 128], P(('tasks', 'rows', 'cols'))
- lengthscale: float32 [1], replicated
- outputscale: float32 [1], replicated
Outputs:
- output: float32 [131072, 128], P(('tasks', 'rows', 'cols'))
All inputs are finite; a program needn't handle non-finite values.
Results may differ from the reference program's by a relative error of at most 0.001.
Values are sent between devices in bfloat16 or wider.
A program may use at most 1 GiB of HBM per device.

```python
import math
import jax
import jax.numpy as jnp
from jax import lax

POINTS = 131072
FEATURES = 128
COLUMNS = 128
ROW_TILE = 2048
COL_TILE = 1024
CLUSTERS = 16


def setup_inputs(seed: int = 0, part: int = 0) -> dict:
    base_key, shared_key = jax.random.split(jax.random.key(seed))
    part_key = jax.random.fold_in(base_key, part)
    k_center, k_label, k_jitter, k_rhs, k_mean = jax.random.split(part_key, 5)
    k_len, k_out = jax.random.split(shared_key)
    feat_scale = 0.7 / math.sqrt(FEATURES)
    centers = jax.random.normal(k_center, (CLUSTERS, FEATURES), jnp.float32) * feat_scale
    labels = jax.random.randint(k_label, (POINTS,), 0, CLUSTERS)
    jitter = jax.random.normal(k_jitter, (POINTS, FEATURES), jnp.float32) * feat_scale
    points = (centers[labels] + jitter).astype(jnp.bfloat16)
    col_mean = jax.random.normal(k_mean, (1, COLUMNS), jnp.float32) / math.sqrt(POINTS)
    rhs_vecs = (jax.random.normal(k_rhs, (POINTS, COLUMNS), jnp.float32) + col_mean).astype(jnp.bfloat16)
    lengthscale = jax.random.uniform(k_len, (1,), jnp.float32, 0.85, 1.15)
    outputscale = jax.random.uniform(k_out, (1,), jnp.float32, 1.0, 2.0) / math.sqrt(POINTS)
    return {'points': points, 'rhs_vecs': rhs_vecs, 'lengthscale': lengthscale, 'outputscale': outputscale}


def reference(points, rhs_vecs, lengthscale, outputscale):
    two_ell_sq = 2.0 * lengthscale[0] * lengthscale[0]
    out_scale = outputscale[0]
    sq_norms = jnp.sum(jnp.square(points.astype(jnp.float32)), axis=1)
    col_pts = points.reshape(POINTS // COL_TILE, COL_TILE, FEATURES)
    col_vecs = rhs_vecs.reshape(POINTS // COL_TILE, COL_TILE, COLUMNS)
    col_norms = sq_norms.reshape(POINTS // COL_TILE, COL_TILE)

    def row_block(row_args):
        row_pts, row_norms = row_args

        def col_step(run_sum, col_blk):
            blk_pts, blk_vecs, blk_norms = col_blk
            gram_mat = jnp.dot(row_pts, blk_pts.T, preferred_element_type=jnp.float32)
            sq_dist = jnp.maximum(row_norms[:, None] + blk_norms[None, :] - 2.0 * gram_mat, 0.0)
            kern_blk = (out_scale * jnp.exp(-sq_dist / two_ell_sq)).astype(jnp.bfloat16)
            return run_sum + jnp.dot(kern_blk, blk_vecs, preferred_element_type=jnp.float32), None

        zero_acc = jnp.zeros((ROW_TILE, COLUMNS), jnp.float32)
        row_sum, _ = lax.scan(col_step, zero_acc, (col_pts, col_vecs, col_norms))
        return row_sum

    row_sums = lax.map(row_block, (points.reshape(POINTS // ROW_TILE, ROW_TILE, FEATURES), sq_norms.reshape(POINTS // ROW_TILE, ROW_TILE)))
    return row_sums.reshape(POINTS, COLUMNS)
```

```python
import functools

import jax
import jax.numpy as jnp
from jax import lax
from jax.experimental import pallas as pl
from jax.experimental.pallas import tpu as pltpu
from jax.sharding import Mesh, PartitionSpec as P

F32 = jnp.float32
BF16 = jnp.bfloat16
BLK = 1024
TILE = 256
BF16_MAX = 3.3895313892515355e38


def split3(n):
    hi = lax.reduce_precision(jnp.minimum(n, BF16_MAX), 8, 7)
    r = n - hi
    mid = lax.reduce_precision(r, 8, 7)
    return hi.astype(BF16), mid.astype(BF16), (r - mid).astype(BF16)


def kernel(nblk, npair, scal_ref, xr_ref, xc_ref, ag_ref, vt_ref, yt_ref):
    negc, logs = scal_ref[0], scal_ref[1]
    cap = jnp.full((TILE, TILE), scal_ref[2], F32).astype(BF16)
    nunit = nblk * npair * 4

    def body(*accs):
        g = (accs[0:2], accs[2:4])
        y = (accs[4:6], accs[6:8])
        for ref in accs:
            pltpu.matmul_pop(ref)
        yt_ref[...] = jnp.zeros_like(yt_ref)

        def where(unit):
            step = unit // 4
            return step // npair, lax.rem(step, npair), lax.rem(unit, 4)

        def gram(unit, par):
            unit = lax.rem(unit, nunit)
            blk, pair, t = where(unit)
            rows = pl.ds(pl.multiple_of(t * TILE, TILE), TILE)
            lhs = jnp.concatenate([xc_ref[blk, rows, :], ag_ref[blk, rows, :]], axis=1)
            for q in range(2):
                cols = pl.ds(pl.multiple_of(pair * (2 * TILE) + q * TILE, TILE), TILE)
                pltpu.matmul_push_rhs(xr_ref[:, cols], 0, q)
                pltpu.matmul_acc_lhs(g[par][q], lhs, load_staged_rhs=0)

        def kern(par, q):
            d = pltpu.matmul_pop(g[par][q])
            k = jnp.exp2(d * negc + logs).astype(BF16)
            return jnp.minimum(k, cap)

        def apply(unit, ks, yp):
            blk, _, t = where(unit)
            lhs = vt_ref[blk, :, pl.ds(pl.multiple_of(t * TILE, TILE), TILE)]
            for q in range(2):
                pltpu.matmul_push_rhs(ks[q], 1, q)
                pltpu.matmul_acc_lhs(y[yp][q], lhs, load_staged_rhs=1)

        def flush(step, yp):
            step = jnp.maximum(step, 0)
            pair = lax.rem(step, npair)
            for q in range(2):
                cols = pl.ds(pl.multiple_of(pair * (2 * TILE) + q * TILE, TILE), TILE)
                yt_ref[:, cols] += pltpu.matmul_pop(y[yp][q])

        gram(0, 0)
        gram(1, 1)

        def trip(i, _):
            for u in range(8):
                unit = i * 8 + u
                ks = [kern(u % 2, q) for q in range(2)]
                gram(unit + 2, u % 2)
                apply(unit, ks, u // 4)
                if u == 2:
                    flush(i * 2 - 1, 1)
                if u == 6:
                    flush(i * 2, 0)
            return 0

        lax.fori_loop(0, nunit // 8, trip, 0)
        flush(nunit // 4 - 1, 1)
        for ref in accs:
            pltpu.matmul_pop(ref)

    acc = lambda q, m: pltpu.ACC(q)((m, TILE), F32)
    pl.run_scoped(body, acc(0, TILE), acc(1, TILE), acc(0, TILE), acc(1, TILE),
                  acc(0, 128), acc(1, 128), acc(0, 128), acc(1, 128))


def solution(mesh):
    grid = Mesh(mesh.devices.reshape(2, 4, 4, 4), ('c', 'z', 'y', 'x'))
    spec = P(('z', 'y', 'x', 'c'), None)

    def per_device(x, v, ell, scale):
        two_ell_sq = 2.0 * ell[0] * ell[0]
        s = scale[0]
        shrink = jnp.where(two_ell_sq > 1.0, 2.0 ** -6, 1.0).astype(F32)
        negc = -(1.4426950408889634 / shrink) / two_ell_sq
        scal = jnp.stack([negc, jnp.log2(jnp.abs(s)), jnp.abs(s)])

        norm = jnp.sum(jnp.square(x.astype(F32)), axis=1)
        pieces = jnp.stack(split3(norm) + (jnp.ones_like(norm, BF16),) * 3)
        aug = jnp.pad(pieces.T, ((0, 0), (0, 122)))
        rowpc = jnp.concatenate([pieces[3:], pieces[:3]], axis=0).astype(F32)
        sb = shrink
        xt = x.T.astype(F32)
        stat = jnp.concatenate([xt * (-2.0 * sb), rowpc * sb, jnp.zeros((122, BLK), F32)], axis=0).astype(BF16)

        xr = lax.all_gather(stat, 'x', axis=1, tiled=True)
        xc = lax.all_gather(x, ('z', 'y', 'c'), axis=0)
        ag = lax.all_gather(aug, ('z', 'y', 'c'), axis=0)
        vt = lax.all_gather(v.T, ('z', 'y', 'c'), axis=0)
        nblk = xc.shape[0]
        npair = xr.shape[1] // (2 * TILE)
        vm = pl.BlockSpec(memory_space=pltpu.VMEM)
        yt = pl.pallas_call(
            functools.partial(kernel, nblk, npair),
            out_shape=jax.ShapeDtypeStruct((128, xr.shape[1]), F32),
            in_specs=[pl.BlockSpec(memory_space=pltpu.SMEM), vm, vm, vm, vm],
            out_specs=vm,
            compiler_params=pltpu.CompilerParams(vmem_limit_bytes=60 * 2 ** 20),
        )(scal, xr, xc, ag, vt)
        part = yt.T * jnp.where(s < 0, -1.0, 1.0)
        return lax.psum_scatter(part, 'x', scatter_dimension=0, tiled=True)

    return jax.shard_map(per_device, mesh=grid, in_specs=(spec, spec, P(None), P(None)), out_specs=spec, check_vma=False)
```

```python
import functools

import jax
import jax.numpy as jnp
from jax import lax
from jax.experimental import pallas as pl
from jax.experimental.pallas import tpu as pltpu
from jax.sharding import Mesh, PartitionSpec as P

F32 = jnp.float32
BF16 = jnp.bfloat16
MESH = pl.DeviceIdType.MESH
BLK = 1024
TILE = 256
HALF = 512
AUG0 = 2 * HALF
ROWS = AUG0 + 4 * 8
XROWS = 144
BF16_MAX = 3.3895313892515355e38

A, B = 0, 1
ORDER = [(0, 0, A), (0, 0, B),
         (0, -1, A), (0, 1, A), (-1, 0, B), (1, 0, B),
         (0, -1, B), (0, 1, B), (-1, 0, A), (1, 0, A),
         (-1, -1, B), (-1, 1, B), (-1, -1, A), (1, -1, A),
         (1, -1, B), (1, 1, B), (-1, 1, A), (1, 1, A),
         (0, 2, A), (2, 0, B), (0, 2, B), (2, 0, A),
         (2, -1, B), (2, 1, B), (-1, 2, A), (1, 2, A),
         (-1, 2, B), (1, 2, B), (2, -1, A), (2, 1, A),
         (2, 2, B), (2, 2, A)]
POS = {key: i for i, key in enumerate(ORDER)}
NPOS = len(ORDER)


def wrap(d):
    return (d + 1) % 4 - 1


def split3(n):
    hi = lax.reduce_precision(jnp.minimum(n, BF16_MAX), 8, 7)
    r = n - hi
    mid = lax.reduce_precision(r, 8, 7)
    return hi.astype(BF16), mid.astype(BF16), (r - mid).astype(BF16)


class Wires:
    def __init__(self, cols, send, ici, d2d, pos):
        self.cols, self.send, self.ici, self.d2d, self.pos = cols, send, ici, d2d, pos
        self.sent = []
        self.dev = {(a, d): {a: lax.rem(pos[a] + d + 4, 4)} for a in 'zyx' for d in (1, -1, 2)}
        self.mate = {'c': 1 - pos['c']}

    def _copy(self, src, dst, recv, dev):
        n = len(self.sent)
        self.sent.append(lambda: pltpu.make_async_copy(src(), src(), self.send.at[n]).wait())
        pltpu.make_async_remote_copy(src_ref=src(), dst_ref=dst(), send_sem=self.send.at[n], recv_sem=recv(),
                                     device_id=dev, device_id_type=MESH).start()

    def block(self, key, c=0, part=None):
        p = POS[key]
        if part is None:
            return lambda: self.cols.at[p, c]
        return lambda: self.cols.at[p, c, pl.ds(part * (ROWS // 2), ROWS // 2)]

    def sem(self, key, part=0):
        return lambda: self.ici.at[POS[key], part]

    def both(self, axis, key):
        for sign in (1, -1):
            dz, dy, h = key
            dst = (dz, wrap(dy - sign), h) if axis == 'y' else (wrap(dz - sign), dy, h)
            self._copy(self.block(key), self.block(dst), self.sem(dst), self.dev[axis, sign])

    def relay(self, axis, off, h):
        dst = (off, 2, h) if axis == 'y' else (2, off, h)
        for part, sign in ((0, 1), (1, -1)):
            src = (off, -sign, h) if axis == 'y' else (-sign, off, h)
            self._copy(self.block(src, 0, part), self.block(dst, 0, part), self.sem(dst, part), self.dev[axis, sign])

    def partner(self, key):
        self._copy(self.block(key, 0), self.block(key, 1), lambda: self.d2d.at[POS[key]], self.mate)

    def _recv(self, dst, sem):
        pltpu.make_async_copy(dst, dst, sem).wait()

    def got(self, key):
        for part in (0, 1) if self.halved(key) else (None,):
            self._recv(self.block(key, 0, part)(), self.sem(key, part or 0)())

    @staticmethod
    def halved(key):
        dz, dy, h = key
        last = (dz if dz != 0 else dy) if h == A else (dy if dy != 0 else dz)
        return last == 2

    def got_partner(self, p):
        self._recv(self.cols.at[p, 1], self.d2d.at[p])


def schedule(w):
    def slot1():
        for key in [(0, -1, A), (0, 1, A), (-1, 0, B), (1, 0, B)]:
            w.got(key)
            w.partner(key)
        for d in (-1, 1):
            w.both('y', (d, 0, B))
            w.both('z', (0, d, A))
        w.relay('y', 0, A)
        w.relay('z', 0, B)

    def slot2():
        for key in [(0, -1, B), (0, 1, B), (-1, 0, A), (1, 0, A)]:
            w.got(key)
            w.partner(key)
        w.relay('y', 0, B)
        w.relay('z', 0, A)

    def slot3():
        for key in [(-1, -1, B), (-1, 1, B), (-1, -1, A), (1, -1, A)]:
            w.got(key)
            w.partner(key)

    def slot4():
        for key in [(0, 2, A), (2, 0, B)]:
            w.got(key)
            w.partner(key)
        w.both('y', (2, 0, B))
        w.both('z', (0, 2, A))
        for key in [(1, -1, B), (1, 1, B), (-1, 1, A), (1, 1, A)]:
            w.got(key)
            w.partner(key)
        for d in (-1, 1):
            w.relay('y', d, B)
            w.relay('z', d, A)

    def slot5():
        for key in [(0, 2, B), (2, 0, A)]:
            w.got(key)
            w.partner(key)

    def slot6():
        for key in [(2, -1, B), (2, 1, B), (-1, 2, A), (1, 2, A)]:
            w.got(key)
            w.partner(key)
        w.relay('y', 2, B)
        w.relay('z', 2, A)

    def slot7():
        for key in [(-1, 2, B), (1, 2, B), (2, -1, A), (2, 1, A)]:
            w.got(key)
            w.partner(key)

    def slot8():
        for key in [(2, 2, B), (2, 2, A)]:
            w.got(key)
            w.partner(key)

    return {1: slot1, 5: slot2, 8: slot3, 9: slot4, 10: slot5, 12: slot6, 14: slot7, 15: slot8}


def kernel(scal_ref, own_ref, xown_ref, out_ref, cols, ag, xr, yt, yin, local, send, ici, d2d, xsem):
    pos = {k: lax.axis_index(k) for k in ('c', 'z', 'y', 'x')}
    w = Wires(cols, send, ici, d2d, pos)
    xdev = lambda d: w.dev['x', d]

    loads = [pltpu.make_async_copy(own_ref.at[h], cols.at[h, 0], local.at[h]) for h in range(2)]
    loads.append(pltpu.make_async_copy(xown_ref, xr.at[0, :, :, pl.ds(0, XROWS)], local.at[2]))
    for cp in loads:
        cp.start()
    barrier = pltpu.get_barrier_semaphore()
    peers = [w.dev[a, d] for a in 'zy' for d in (1, -1)] + [xdev(1), xdev(-1), xdev(2), w.mate]
    for dev in peers:
        pl.semaphore_signal(barrier, inc=1, device_id=dev, device_id_type=MESH)
    xr[:, :, :, pl.ds(XROWS, TILE - XROWS), :] = jnp.zeros((4, 4, 2, TILE - XROWS, 128), BF16)
    yt[...] = jnp.zeros_like(yt)
    for cp in loads:
        cp.wait()
    pl.semaphore_wait(barrier, len(peers))

    def xcopy(src, dst, tiles, recv, d):
        cut = lambda b: lambda: xr.at[b, pl.ds(*tiles), :, pl.ds(0, XROWS)]
        w._copy(cut(src), cut(dst), lambda: xsem.at[recv], xdev(d))

    def xgot(dst, tiles, recv):
        ref = xr.at[dst, pl.ds(*tiles), :, pl.ds(0, XROWS)]
        pltpu.make_async_copy(ref, ref, xsem.at[recv]).wait()

    w.partner((0, 0, A))
    w.partner((0, 0, B))
    xcopy(0, 1, (0, 4), 0, 1)
    xcopy(0, 2, (0, 4), 1, -1)
    w.both('y', (0, 0, A))
    w.both('z', (0, 0, B))
    w.both('y', (0, 0, B))
    w.both('z', (0, 0, A))

    negc, logs = scal_ref[0], scal_ref[1]

    def build(p, c, tiles):
        for lt in tiles:
            piece = cols[p, c, pl.ds(AUG0 + lt * 8, 8), :].astype(F32)
            full = jnp.concatenate([piece, jnp.zeros((120, 128), F32)], axis=0)
            ag[p, c, pl.ds(lt * 128, 128), :] = full.T.astype(BF16)

    def work(p, xb, pair):
        lhs = jnp.concatenate([jnp.concatenate([cols[p, c, pl.ds(0, HALF), :], ag[p, c]], axis=1) for c in range(2)], axis=0)
        rhs = jnp.concatenate([jnp.concatenate([xr[xb, pair * 2 + q, h] for h in range(2)], axis=1) for q in range(2)], axis=1)
        dist = jnp.dot(lhs, rhs, preferred_element_type=F32)
        kern = jnp.exp2(dist * negc + logs).astype(BF16)
        kern = jnp.minimum(kern, jnp.full(kern.shape, scal_ref[2], F32).astype(BF16))
        vt = jnp.concatenate([cols[p, c, pl.ds(HALF + 128 * k, 128), :] for c in range(2) for k in range(4)], axis=1)
        return jnp.dot(vt, kern, preferred_element_type=F32)

    def add(xb, pair, r):
        for q in range(2):
            yt[xb, pair * 2 + q] += r[:, q * TILE:(q + 1) * TILE]

    acts = schedule(w)

    def phase_a(i, _):
        p, h = lax.div(i, 2), lax.rem(i, 2)

        @pl.when(h == 0)
        def _():
            for at, act in acts.items():
                pl.when(p == at)(act)

        @pl.when(i == 1)
        def _():
            xgot(3, (0, 2), 2)
            xgot(3, (2, 2), 3)

        @pl.when((h == 1) & (p > 0))
        def _():
            w.got_partner(p + 1)

        for k in range(2):
            for pair in range(2):
                add(2 * h + k, pair, work(p, 2 * h + k, pair))
        build(p + 1, h, range(4))
        return 0

    def phase_b1(i, _):
        p = 16 + 2 * i

        @pl.when(i < 7)
        def _():
            w.got_partner(p + 2)
            w.got_partner(p + 3)

        for pair in range(2):
            add(3, pair, work(p, 3, pair) + work(p + 1, 3, pair))
        for k in range(2):
            for c in range(2):
                build(16 + lax.rem(2 * i + 2 + k, 16), c, range(4))
        return 0

    def ysend(label, d, slot):
        return lambda: pltpu.make_async_remote_copy(src_ref=yt.at[label], dst_ref=yin.at[slot], send_sem=xsem.at[4 + slot],
                                                    recv_sem=xsem.at[7 + slot], device_id=xdev(d), device_id_type=MESH)

    sends = [ysend(3, 2, 2), ysend(2, 1, 0), ysend(1, -1, 1)]

    def phase_b2(i, _):
        for n in range(3):
            pl.when(i == 8 * n + 1)(lambda n=n: sends[n]().start())
        xb, p = 2 - lax.div(i, 8), 16 + 2 * lax.rem(i, 8)
        for pair in range(2):
            add(xb, pair, work(p, xb, pair) + work(p + 1, xb, pair))
        return 0

    for p in range(2):
        w.got_partner(p)
        if p == 0:
            for c in range(2):
                build(p, c, range(4))
    xgot(1, (0, 4), 0)
    xgot(2, (0, 4), 1)
    xcopy(1, 3, (0, 2), 2, 1)
    xcopy(2, 3, (2, 2), 3, -1)
    lax.fori_loop(0, 32, phase_a, 0)
    w.got_partner(17)
    for c in range(2):
        build(17, c, range(4))
    lax.fori_loop(0, 8, phase_b1, 0)
    lax.fori_loop(0, 24, phase_b2, 0)
    for cp in sends:
        cp().wait()
    for wait in w.sent:
        wait()
    for t in range(4):
        total = (yt[0, t] + yin[0, t] + yin[1, t] + yin[2, t]) * scal_ref[3]
        out_ref[pl.ds(t * TILE, TILE), :] = total.T


def solution(mesh):
    grid = Mesh(mesh.devices.reshape(2, 4, 4, 4), ('c', 'z', 'y', 'x'))
    spec = P(('z', 'y', 'x', 'c'), None)

    def per_device(x, v, ell, scale):
        two_ell_sq = 2.0 * ell[0] * ell[0]
        s = scale[0]
        shrink = jnp.where(two_ell_sq > 1.0, 2.0 ** -6, 1.0).astype(F32)
        negc = -(1.4426950408889634 / shrink) / two_ell_sq
        scal = jnp.stack([negc, jnp.log2(jnp.abs(s)), jnp.abs(s), jnp.where(s < 0, -1.0, 1.0)])

        norm = jnp.sum(jnp.square(x.astype(F32)), axis=1)
        pieces = jnp.stack(split3(norm) + (jnp.ones_like(norm, BF16),) * 3)
        lanes = jnp.pad(pieces, ((0, 2), (0, 0))).reshape(8, 8, 128).transpose(1, 0, 2)
        vt = v.reshape(8, 128, 128).transpose(0, 2, 1)
        own = jnp.concatenate([x.reshape(2, HALF, 128), vt.reshape(2, HALF, 128), lanes.reshape(2, 32, 128)], axis=1)

        xt = x.reshape(4, 2, 128, 128).transpose(0, 1, 3, 2).astype(F32) * (-2.0 * shrink)
        rowpc = jnp.pad(jnp.concatenate([pieces[3:], pieces[:3]]).astype(F32) * shrink, ((0, 10), (0, 0)))
        rowpc = rowpc.reshape(16, 4, 2, 128).transpose(1, 2, 0, 3)
        xown = jnp.concatenate([xt, rowpc], axis=2).astype(BF16)

        anym = pl.BlockSpec(memory_space=pl.ANY)
        return pl.pallas_call(
            kernel,
            out_shape=jax.ShapeDtypeStruct((BLK, 128), F32),
            name='comm',
            in_specs=[pl.BlockSpec(memory_space=pltpu.SMEM), anym, anym],
            out_specs=pl.BlockSpec(memory_space=pltpu.VMEM),
            scratch_shapes=[
                pltpu.VMEM((NPOS, 2, ROWS, 128), BF16),
                pltpu.VMEM((NPOS, 2, HALF, 128), BF16),
                pltpu.VMEM((4, 4, 2, TILE, 128), BF16),
                pltpu.VMEM((4, 4, 128, TILE), F32),
                pltpu.VMEM((3, 4, 128, TILE), F32),
                pltpu.SemaphoreType.DMA((3,)),
                pltpu.SemaphoreType.DMA((100,)),
                pltpu.SemaphoreType.DMA((NPOS, 2)),
                pltpu.SemaphoreType.DMA((NPOS,)),
                pltpu.SemaphoreType.DMA((10,)),
            ],
            compiler_params=pltpu.CompilerParams(vmem_limit_bytes=60 * 2 ** 20, collective_id=0, has_side_effects=True),
        )(scal, own, xown)

    return jax.shard_map(per_device, mesh=grid, in_specs=(spec, spec, P(None), P(None)), out_specs=spec, check_vma=False)
```

```python
import functools

import jax
import jax.numpy as jnp
from jax import lax
from jax.experimental import pallas as pl
from jax.experimental.pallas import tpu as pltpu
from jax.sharding import Mesh, PartitionSpec as P

F32 = jnp.float32
BF16 = jnp.bfloat16
MESH = pl.DeviceIdType.MESH
BLK = 1024
TILE = 256
HALF = 512
AUG0 = 2 * HALF
ROWS = AUG0 + 4 * 8
XROWS = 144
BF16_MAX = 3.3895313892515355e38

A, B = 0, 1
ORDER = [(0, 0, A), (0, 0, B),
         (0, -1, A), (0, 1, A), (-1, 0, B), (1, 0, B),
         (0, -1, B), (0, 1, B), (-1, 0, A), (1, 0, A),
         (-1, -1, B), (-1, 1, B), (-1, -1, A), (1, -1, A),
         (1, -1, B), (1, 1, B), (-1, 1, A), (1, 1, A),
         (0, 2, A), (2, 0, B), (0, 2, B), (2, 0, A),
         (2, -1, B), (2, 1, B), (-1, 2, A), (1, 2, A),
         (-1, 2, B), (1, 2, B), (2, -1, A), (2, 1, A),
         (2, 2, B), (2, 2, A)]
POS = {key: i for i, key in enumerate(ORDER)}
NPOS = len(ORDER)


def wrap(d):
    return (d + 1) % 4 - 1


def split3(n):
    hi = lax.reduce_precision(jnp.minimum(n, BF16_MAX), 8, 7)
    r = n - hi
    mid = lax.reduce_precision(r, 8, 7)
    return hi.astype(BF16), mid.astype(BF16), (r - mid).astype(BF16)


class Wires:
    def __init__(self, cols, send, ici, d2d, pos):
        self.cols, self.send, self.ici, self.d2d, self.pos = cols, send, ici, d2d, pos
        self.sent = []
        self.dev = {(a, d): {a: lax.rem(pos[a] + d + 4, 4)} for a in 'zyx' for d in (1, -1, 2)}
        self.mate = {'c': 1 - pos['c']}

    def _copy(self, src, dst, recv, dev):
        n = len(self.sent)
        self.sent.append(lambda: pltpu.make_async_copy(src(), src(), self.send.at[n]).wait())
        pltpu.make_async_remote_copy(src_ref=src(), dst_ref=dst(), send_sem=self.send.at[n], recv_sem=recv(),
                                     device_id=dev, device_id_type=MESH).start()

    def block(self, key, c=0, part=None):
        p = POS[key]
        if part is None:
            return lambda: self.cols.at[p, c]
        return lambda: self.cols.at[p, c, pl.ds(part * (ROWS // 2), ROWS // 2)]

    def sem(self, key, part=0):
        return lambda: self.ici.at[POS[key], part]

    def both(self, axis, key):
        for sign in (1, -1):
            dz, dy, h = key
            dst = (dz, wrap(dy - sign), h) if axis == 'y' else (wrap(dz - sign), dy, h)
            self._copy(self.block(key), self.block(dst), self.sem(dst), self.dev[axis, sign])

    def relay(self, axis, off, h):
        dst = (off, 2, h) if axis == 'y' else (2, off, h)
        for part, sign in ((0, 1), (1, -1)):
            src = (off, -sign, h) if axis == 'y' else (-sign, off, h)
            self._copy(self.block(src, 0, part), self.block(dst, 0, part), self.sem(dst, part), self.dev[axis, sign])

    def partner(self, key):
        self._copy(self.block(key, 0), self.block(key, 1), lambda: self.d2d.at[POS[key]], self.mate)

    def _recv(self, dst, sem):
        pltpu.make_async_copy(dst, dst, sem).wait()

    def got(self, key):
        for part in (0, 1) if self.halved(key) else (None,):
            self._recv(self.block(key, 0, part)(), self.sem(key, part or 0)())

    @staticmethod
    def halved(key):
        dz, dy, h = key
        last = (dz if dz != 0 else dy) if h == A else (dy if dy != 0 else dz)
        return last == 2

    def got_partner(self, p):
        self._recv(self.cols.at[p, 1], self.d2d.at[p])


def schedule(w):
    def slot1():
        for key in [(0, -1, A), (0, 1, A), (-1, 0, B), (1, 0, B)]:
            w.got(key)
            w.partner(key)
        for d in (-1, 1):
            w.both('y', (d, 0, B))
            w.both('z', (0, d, A))
        w.relay('y', 0, A)
        w.relay('z', 0, B)

    def slot2():
        for key in [(0, -1, B), (0, 1, B), (-1, 0, A), (1, 0, A)]:
            w.got(key)
            w.partner(key)
        w.relay('y', 0, B)
        w.relay('z', 0, A)

    def slot3():
        for key in [(-1, -1, B), (-1, 1, B), (-1, -1, A), (1, -1, A)]:
            w.got(key)
            w.partner(key)

    def slot4():
        for key in [(0, 2, A), (2, 0, B)]:
            w.got(key)
            w.partner(key)
        w.both('y', (2, 0, B))
        w.both('z', (0, 2, A))
        for key in [(1, -1, B), (1, 1, B), (-1, 1, A), (1, 1, A)]:
            w.got(key)
            w.partner(key)
        for d in (-1, 1):
            w.relay('y', d, B)
            w.relay('z', d, A)

    def slot5():
        for key in [(0, 2, B), (2, 0, A)]:
            w.got(key)
            w.partner(key)

    def slot6():
        for key in [(2, -1, B), (2, 1, B), (-1, 2, A), (1, 2, A)]:
            w.got(key)
            w.partner(key)
        w.relay('y', 2, B)
        w.relay('z', 2, A)

    def slot7():
        for key in [(-1, 2, B), (1, 2, B), (2, -1, A), (2, 1, A)]:
            w.got(key)
            w.partner(key)

    def slot8():
        for key in [(2, 2, B), (2, 2, A)]:
            w.got(key)
            w.partner(key)

    return {1: slot1, 4: slot2, 8: slot3, 9: slot4, 10: slot5, 12: slot6, 14: slot7, 15: slot8}


def kernel(scal_ref, own_ref, xown_ref, out_ref, cols, ag, xr, yt, yin, local, send, ici, d2d, xsem, ysem):
    pos = {k: lax.axis_index(k) for k in ('c', 'z', 'y', 'x')}
    w = Wires(cols, send, ici, d2d, pos)
    xdev = lambda d: w.dev['x', d]

    loads = [pltpu.make_async_copy(own_ref.at[h], cols.at[h, 0], local.at[h]) for h in range(2)]
    loads.append(pltpu.make_async_copy(xown_ref, xr.at[0, :, :, pl.ds(0, XROWS)], local.at[2]))
    for cp in loads:
        cp.start()
    barrier = pltpu.get_barrier_semaphore()
    peers = [w.dev[a, d] for a in 'zy' for d in (1, -1)] + [xdev(1), xdev(-1), xdev(2), w.mate]
    for dev in peers:
        pl.semaphore_signal(barrier, inc=1, device_id=dev, device_id_type=MESH)
    xr[:, :, :, pl.ds(XROWS, TILE - XROWS), :] = jnp.zeros((4, 4, 2, TILE - XROWS, 128), BF16)
    yt[...] = jnp.zeros_like(yt)
    for cp in loads:
        cp.wait()
    pl.semaphore_wait(barrier, len(peers))

    def xcopy(src, dst, tiles, recv, d):
        cut = lambda b: lambda: xr.at[b, pl.ds(*tiles), :, pl.ds(0, XROWS)]
        w._copy(cut(src), cut(dst), lambda: xsem.at[recv], xdev(d))

    def xgot(dst, tiles, recv):
        ref = xr.at[dst, pl.ds(*tiles), :, pl.ds(0, XROWS)]
        pltpu.make_async_copy(ref, ref, xsem.at[recv]).wait()

    w.partner((0, 0, A))
    w.partner((0, 0, B))
    xcopy(0, 1, (0, 4), 0, 1)
    xcopy(0, 2, (0, 4), 1, -1)
    w.both('y', (0, 0, A))
    w.both('z', (0, 0, B))
    w.both('y', (0, 0, B))
    w.both('z', (0, 0, A))

    negc, logs = scal_ref[0], scal_ref[1]

    def build(p, c, tiles):
        for lt in tiles:
            piece = cols[p, c, pl.ds(AUG0 + lt * 8, 8), :].astype(F32)
            full = jnp.concatenate([piece, jnp.zeros((120, 128), F32)], axis=0)
            ag[p, c, pl.ds(lt * 128, 128), :] = full.T.astype(BF16)

    def work(p, xb, pair):
        lhs = jnp.concatenate([jnp.concatenate([cols[p, c, pl.ds(0, HALF), :], ag[p, c]], axis=1) for c in range(2)], axis=0)
        rhs = jnp.concatenate([jnp.concatenate([xr[xb, pair * 2 + q, h] for h in range(2)], axis=1) for q in range(2)], axis=1)
        dist = jnp.dot(lhs, rhs, preferred_element_type=F32)
        kern = jnp.exp2(dist * negc + logs).astype(BF16)
        kern = jnp.minimum(kern, jnp.full(kern.shape, scal_ref[2], F32).astype(BF16))
        vt = jnp.concatenate([cols[p, c, pl.ds(HALF + 128 * k, 128), :] for c in range(2) for k in range(4)], axis=1)
        return jnp.dot(vt, kern, preferred_element_type=F32)

    def add(xb, pair, r):
        for q in range(2):
            yt[xb, pair * 2 + q] += r[:, q * TILE:(q + 1) * TILE]

    acts = schedule(w)

    def phase_a(i, _):
        p, h = lax.div(i, 2), lax.rem(i, 2)

        @pl.when(h == 0)
        def _():
                pl.when(p == 1)(acts[1])

        @pl.when(i == 1)
        def _():
            xgot(3, (0, 2), 2)
            xgot(3, (2, 2), 3)

        @pl.when((h == 1) & (p > 0))
        def _():
            w.got_partner(p + 1)

        for k in range(2):
            for pair in range(2):
                add(2 * h + k, pair, work(p, 2 * h + k, pair))
        build(p + 1, h, range(4))
        return 0

    def phase_a4(n, _):
        p = n + 2
        for at, act in acts.items():
            if at > 1:
                pl.when(p == at)(act)
        w.got_partner(p + 1)
        late = p + lax.div(p, 12) * (5 - 3 * lax.div(p, 15))
        pl.when((p >= 12) & (p < 15))(lambda: w.got_partner(p + 5))
        for xb in range(4):
            for pair in range(2):
                add(xb, pair, work(p, xb, pair))
        for c in range(2):
            build(p + 1, c, range(4))
            build(late, c, range(4))
        return 0

    def sweep(xb, i):
        p = 16 + 4 * i
        for pair in range(2):
            add(xb, pair, sum(work(p + k, xb, pair) for k in range(4)))

    def phase_b1(i, _):
        @pl.when(i < 3)
        def _():
            for k in range(4):
                w.got_partner(20 + 4 * i + k)

        sweep(3, i)
        for k in range(4):
            for c in range(2):
                build(16 + lax.rem(4 * i + 4 + k, 16), c, range(4))
        return 0

    def ysend(label, d, slot, pair):
        tiles = pl.ds(2 * pair, 2)
        return lambda: pltpu.make_async_remote_copy(
            src_ref=yt.at[label, tiles], dst_ref=yin.at[slot, tiles], send_sem=ysem.at[0, slot, pair],
            recv_sem=ysem.at[1, slot, pair], device_id=xdev(d), device_id_type=MESH)

    sends = [[ysend(*who, pair) for pair in range(2)] for who in ((3, 2, 2), (2, 1, 0), (1, -1, 1))]

    def phase_b2(i, _):
        for n in range(3):
            for pair in range(2):
                pl.when(i == 4 * n + pair)(lambda n=n, pair=pair: sends[n][pair]().start())
        sweep(2 - lax.div(i, 4), lax.rem(i, 4))
        return 0

    for p in range(2):
        w.got_partner(p)
        if p == 0:
            for c in range(2):
                build(p, c, range(4))
    xgot(1, (0, 4), 0)
    xgot(2, (0, 4), 1)
    xcopy(1, 3, (0, 2), 2, 1)
    xcopy(2, 3, (2, 2), 3, -1)
    lax.fori_loop(0, 4, phase_a, 0)
    lax.fori_loop(0, 14, phase_a4, 0)
    lax.fori_loop(0, 4, phase_b1, 0)
    lax.fori_loop(0, 12, phase_b2, 0)
    for pairs in sends:
        for cp in pairs:
            cp().wait()
    for wait in w.sent:
        wait()
    for t in range(4):
        total = (yt[0, t] + yin[0, t] + yin[1, t] + yin[2, t]) * scal_ref[3]
        out_ref[pl.ds(t * TILE, TILE), :] = total.T


def solution(mesh):
    grid = Mesh(mesh.devices.reshape(2, 4, 4, 4), ('c', 'z', 'y', 'x'))
    spec = P(('z', 'y', 'x', 'c'), None)

    def per_device(x, v, ell, scale):
        two_ell_sq = 2.0 * ell[0] * ell[0]
        s = scale[0]
        shrink = jnp.where(two_ell_sq > 1.0, 2.0 ** -6, 1.0).astype(F32)
        negc = -(1.4426950408889634 / shrink) / two_ell_sq
        scal = jnp.stack([negc, jnp.log2(jnp.abs(s)), jnp.abs(s), jnp.where(s < 0, -1.0, 1.0)])

        norm = jnp.sum(jnp.square(x.astype(F32)), axis=1)
        pieces = jnp.stack(split3(norm) + (jnp.ones_like(norm, BF16),) * 3)
        lanes = jnp.pad(pieces, ((0, 2), (0, 0))).reshape(8, 8, 128).transpose(1, 0, 2)
        vt = v.reshape(8, 128, 128).transpose(0, 2, 1)
        own = jnp.concatenate([x.reshape(2, HALF, 128), vt.reshape(2, HALF, 128), lanes.reshape(2, 32, 128)], axis=1)

        xt = x.reshape(4, 2, 128, 128).transpose(0, 1, 3, 2).astype(F32) * (-2.0 * shrink)
        rowpc = jnp.pad(jnp.concatenate([pieces[3:], pieces[:3]]).astype(F32) * shrink, ((0, 10), (0, 0)))
        rowpc = rowpc.reshape(16, 4, 2, 128).transpose(1, 2, 0, 3)
        xown = jnp.concatenate([xt, rowpc], axis=2).astype(BF16)

        anym = pl.BlockSpec(memory_space=pl.ANY)
        return pl.pallas_call(
            kernel,
            out_shape=jax.ShapeDtypeStruct((BLK, 128), F32),
            name='comm',
            in_specs=[pl.BlockSpec(memory_space=pltpu.SMEM), anym, anym],
            out_specs=pl.BlockSpec(memory_space=pltpu.VMEM),
            scratch_shapes=[
                pltpu.VMEM((NPOS, 2, ROWS, 128), BF16),
                pltpu.VMEM((NPOS, 2, HALF, 128), BF16),
                pltpu.VMEM((4, 4, 2, TILE, 128), BF16),
                pltpu.VMEM((4, 4, 128, TILE), F32),
                pltpu.VMEM((3, 4, 128, TILE), F32),
                pltpu.SemaphoreType.DMA((3,)),
                pltpu.SemaphoreType.DMA((100,)),
                pltpu.SemaphoreType.DMA((NPOS, 2)),
                pltpu.SemaphoreType.DMA((NPOS,)),
                pltpu.SemaphoreType.DMA((4,)),
                pltpu.SemaphoreType.DMA((2, 3, 2)),
            ],
            compiler_params=pltpu.CompilerParams(vmem_limit_bytes=60 * 2 ** 20, collective_id=0, has_side_effects=True),
        )(scal, own, xown)

    return jax.shard_map(per_device, mesh=grid, in_specs=(spec, spec, P(None), P(None)), out_specs=spec, check_vma=False)
```

```python
import functools

import jax
import jax.numpy as jnp
from jax import lax
from jax.experimental import pallas as pl
from jax.experimental.pallas import tpu as pltpu
from jax.sharding import Mesh, PartitionSpec as P

F32 = jnp.float32
BF16 = jnp.bfloat16
MESH = pl.DeviceIdType.MESH
BLK = 1024
TILE = 256
HALF = 512
AUG0 = 2 * HALF
ROWS = AUG0 + 4 * 8
XROWS = 144
BF16_MAX = 3.3895313892515355e38

A, B = 0, 1
ORDER = [(0, 0, A), (0, 0, B),
         (0, -1, A), (0, 1, A), (-1, 0, B), (1, 0, B),
         (0, -1, B), (0, 1, B), (-1, 0, A), (1, 0, A),
         (-1, -1, B), (-1, 1, B), (-1, -1, A), (1, -1, A),
         (1, -1, B), (1, 1, B), (-1, 1, A), (1, 1, A),
         (0, 2, A), (2, 0, B), (0, 2, B), (2, 0, A),
         (2, -1, B), (2, 1, B), (-1, 2, A), (1, 2, A),
         (-1, 2, B), (1, 2, B), (2, -1, A), (2, 1, A),
         (2, 2, B), (2, 2, A)]
POS = {key: i for i, key in enumerate(ORDER)}
NPOS = len(ORDER)


def wrap(d):
    return (d + 1) % 4 - 1


def split3(n):
    hi = jnp.minimum(n, BF16_MAX).astype(BF16).astype(F32)
    r = n - hi
    mid = r.astype(BF16).astype(F32)
    return hi, mid, r - mid


class Wires:
    def __init__(self, cols, send, ici, d2d, pos):
        self.cols, self.send, self.ici, self.d2d, self.pos = cols, send, ici, d2d, pos
        self.sent = []
        self.dev = {(a, d): {a: lax.rem(pos[a] + d + 4, 4)} for a in 'zyx' for d in (1, -1, 2)}
        self.mate = {'c': 1 - pos['c']}

    def _copy(self, src, dst, recv, dev):
        n = len(self.sent)
        self.sent.append(lambda: pltpu.make_async_copy(src(), src(), self.send.at[n]).wait())
        pltpu.make_async_remote_copy(src_ref=src(), dst_ref=dst(), send_sem=self.send.at[n], recv_sem=recv(),
                                     device_id=dev, device_id_type=MESH).start()

    def block(self, key, c=0, part=None):
        p = POS[key]
        if part is None:
            return lambda: self.cols.at[p, c]
        return lambda: self.cols.at[p, c, pl.ds(part * (ROWS // 2), ROWS // 2)]

    def sem(self, key, part=0):
        return lambda: self.ici.at[POS[key], part]

    def both(self, axis, key):
        for sign in (1, -1):
            dz, dy, h = key
            dst = (dz, wrap(dy - sign), h) if axis == 'y' else (wrap(dz - sign), dy, h)
            self._copy(self.block(key), self.block(dst), self.sem(dst), self.dev[axis, sign])

    def relay(self, axis, off, h):
        dst = (off, 2, h) if axis == 'y' else (2, off, h)
        for part, sign in ((0, 1), (1, -1)):
            src = (off, -sign, h) if axis == 'y' else (-sign, off, h)
            self._copy(self.block(src, 0, part), self.block(dst, 0, part), self.sem(dst, part), self.dev[axis, sign])

    def partner(self, key):
        self._copy(self.block(key, 0), self.block(key, 1), lambda: self.d2d.at[POS[key]], self.mate)

    def _recv(self, dst, sem):
        pltpu.make_async_copy(dst, dst, sem).wait()

    def got(self, key):
        for part in (0, 1) if self.halved(key) else (None,):
            self._recv(self.block(key, 0, part)(), self.sem(key, part or 0)())

    @staticmethod
    def halved(key):
        dz, dy, h = key
        last = (dz if dz != 0 else dy) if h == A else (dy if dy != 0 else dz)
        return last == 2

    def got_partner(self, p):
        self._recv(self.cols.at[p, 1], self.d2d.at[p])


def schedule(w):
    def slot1():
        for key in [(0, -1, A), (0, 1, A), (-1, 0, B), (1, 0, B)]:
            w.got(key)
            w.partner(key)
        for d in (-1, 1):
            w.both('y', (d, 0, B))
            w.both('z', (0, d, A))
        w.relay('y', 0, A)
        w.relay('z', 0, B)

    def slot2():
        for key in [(0, -1, B), (0, 1, B), (-1, 0, A), (1, 0, A)]:
            w.got(key)
            w.partner(key)
        w.relay('y', 0, B)
        w.relay('z', 0, A)

    def slot3():
        for key in [(-1, -1, B), (-1, 1, B), (-1, -1, A), (1, -1, A)]:
            w.got(key)
            w.partner(key)

    def slot4():
        for key in [(0, 2, A), (2, 0, B)]:
            w.got(key)
            w.partner(key)
        w.both('y', (2, 0, B))
        w.both('z', (0, 2, A))
        for key in [(1, -1, B), (1, 1, B), (-1, 1, A), (1, 1, A)]:
            w.got(key)
            w.partner(key)
        for d in (-1, 1):
            w.relay('y', d, B)
            w.relay('z', d, A)

    def slot5():
        for key in [(0, 2, B), (2, 0, A)]:
            w.got(key)
            w.partner(key)

    def slot6():
        for key in [(2, -1, B), (2, 1, B), (-1, 2, A), (1, 2, A)]:
            w.got(key)
            w.partner(key)
        w.relay('y', 2, B)
        w.relay('z', 2, A)

    def slot7():
        for key in [(-1, 2, B), (1, 2, B), (2, -1, A), (2, 1, A)]:
            w.got(key)
            w.partner(key)

    def slot8():
        for key in [(2, 2, B), (2, 2, A)]:
            w.got(key)
            w.partner(key)

    return {1: slot1, 4: slot2, 8: slot3, 9: slot4, 10: slot5, 12: slot6, 14: slot7, 15: slot8}


def kernel(ell_ref, scale_ref, x_ref, v_ref, out_ref, cols, ag, xr, yt, yin, vbuf, local, send, ici, d2d, xsem, ysem):
    pos = {k: lax.axis_index(k) for k in ('c', 'z', 'y', 'x')}
    w = Wires(cols, send, ici, d2d, pos)
    xdev = lambda d: w.dev['x', d]

    loads = [pltpu.make_async_copy(x_ref.at[pl.ds(h * HALF, HALF)], cols.at[h, 0, pl.ds(0, HALF)], local.at[h]) for h in range(2)]
    loads.append(pltpu.make_async_copy(v_ref, vbuf, local.at[2]))
    for cp in loads:
        cp.start()
    barrier = pltpu.get_barrier_semaphore()
    peers = [w.dev[a, d] for a in 'zy' for d in (1, -1)] + [xdev(1), xdev(-1), xdev(2), w.mate]
    for dev in peers:
        pl.semaphore_signal(barrier, inc=1, device_id=dev, device_id_type=MESH)
    xr[:, :, :, pl.ds(XROWS, TILE - XROWS), :] = jnp.zeros((4, 4, 2, TILE - XROWS, 128), BF16)
    yt[...] = jnp.zeros_like(yt)

    ell = jnp.full((8, 128), ell_ref[0], F32)
    size = jnp.abs(jnp.full((8, 128), scale_ref[0], F32))
    two_ell_sq = 2.0 * ell * ell
    shrink = jnp.where(two_ell_sq > 1.0, 2.0 ** -6, 1.0)
    negc = (-(1.4426950408889634 / shrink) / two_ell_sq)[0, 0]
    logs = jnp.log2(size)[0, 0]
    cap = size[0, 0]
    shrink = shrink[0, 0]

    for cp in loads:
        cp.wait()
    for t in range(8):
        half, at = t // 4, (t % 4) * 128
        xt = cols[half, 0, pl.ds(at, 128), :].astype(F32).T
        hi, mid, lo = split3(jnp.sum(xt * xt, axis=0, keepdims=True))
        row = lax.broadcasted_iota(jnp.int32, (16, 128), 0)
        ones = jnp.where(row < 6, 1.0, 0.0)
        left = jnp.where(row == 0, hi, jnp.where(row == 1, mid, jnp.where(row == 2, lo, ones)))
        right = jnp.where(row == 3, hi, jnp.where(row == 4, mid, jnp.where(row == 5, lo, ones)))
        cols[half, 0, pl.ds(AUG0 + (t % 4) * 8, 8), :] = left[:8].astype(BF16)
        xr[0, t // 2, t % 2, pl.ds(0, 128), :] = (xt * (-2.0 * shrink)).astype(BF16)
        xr[0, t // 2, t % 2, pl.ds(128, 16), :] = (right * shrink).astype(BF16)
        cols[half, 0, pl.ds(HALF + at, 128), :] = vbuf[pl.ds(t * 128, 128), :].astype(F32).T.astype(BF16)
    pl.semaphore_wait(barrier, len(peers))

    def xcopy(src, dst, tiles, recv, d):
        cut = lambda b: lambda: xr.at[b, pl.ds(*tiles), :, pl.ds(0, XROWS)]
        w._copy(cut(src), cut(dst), lambda: xsem.at[recv], xdev(d))

    def xgot(dst, tiles, recv):
        ref = xr.at[dst, pl.ds(*tiles), :, pl.ds(0, XROWS)]
        pltpu.make_async_copy(ref, ref, xsem.at[recv]).wait()

    w.partner((0, 0, A))
    w.partner((0, 0, B))
    for part in range(2):
        xcopy(0, 1, (2 * part, 2), part, 1)
        xcopy(0, 2, (2 * part, 2), 2 + part, -1)
    w.both('y', (0, 0, A))
    w.both('z', (0, 0, B))
    w.both('y', (0, 0, B))
    w.both('z', (0, 0, A))

    def build(p, c, tiles):
        for lt in tiles:
            piece = cols[p, c, pl.ds(AUG0 + lt * 8, 8), :].astype(F32)
            full = jnp.concatenate([piece, jnp.zeros((120, 128), F32)], axis=0)
            ag[p, c, pl.ds(lt * 128, 128), :] = full.T.astype(BF16)

    def work(p, xb, pair):
        lhs = jnp.concatenate([jnp.concatenate([cols[p, c, pl.ds(0, HALF), :], ag[p, c]], axis=1) for c in range(2)], axis=0)
        rhs = jnp.concatenate([jnp.concatenate([xr[xb, pair * 2 + q, h] for h in range(2)], axis=1) for q in range(2)], axis=1)
        dist = jnp.dot(lhs, rhs, preferred_element_type=F32)
        kern = jnp.exp2(dist * negc + logs).astype(BF16)
        kern = jnp.minimum(kern, jnp.full(kern.shape, cap, F32).astype(BF16))
        vt = jnp.concatenate([cols[p, c, pl.ds(HALF + 128 * k, 128), :] for c in range(2) for k in range(4)], axis=1)
        return jnp.dot(vt, kern, preferred_element_type=F32)

    def add(xb, pair, r):
        for q in range(2):
            yt[xb, pair * 2 + q] += r[:, q * TILE:(q + 1) * TILE]

    acts = schedule(w)

    def phase_0(k, _):
        @pl.when(k == 2)
        def _():
            xgot(1, (0, 2), 0)

        @pl.when(k == 3)
        def _():
            xgot(2, (0, 2), 2)
            xcopy(1, 3, (0, 2), 4, 1)

        @pl.when(k == 4)
        def _():
            xgot(1, (2, 2), 1)

        @pl.when(k == 5)
        def _():
            xgot(2, (2, 2), 3)
            xcopy(2, 3, (2, 2), 5, -1)
            acts[1]()

        @pl.when(k == 6)
        def _():
            xgot(3, (0, 2), 4)

        @pl.when(k == 7)
        def _():
            xgot(3, (2, 2), 5)
            w.got_partner(2)

        a, b = lax.div(k, 2), lax.rem(k, 2)
        e = lax.div(a + 1, 2)
        inner = lax.rem(e, 2)
        xb = inner * (1 + b) + (1 - inner) * 3 * lax.div(e, 2)
        pair = inner * (a - 1) + (1 - inner) * b
        add(xb, pair, work(0, xb, pair) + work(1, xb, pair))
        for c in range(2):
            build(1 + lax.div(k, 7), c, range(4))
        return 0

    def phase_a4(n, _):
        p = n + 2
        for at, act in acts.items():
            if at > 1:
                pl.when(p == at)(act)
        w.got_partner(p + 1)
        late = p + lax.div(p, 12) * (5 - 3 * lax.div(p, 15))
        pl.when((p >= 12) & (p < 15))(lambda: w.got_partner(p + 5))
        for xb in range(4):
            for pair in range(2):
                add(xb, pair, work(p, xb, pair))
        for c in range(2):
            build(p + 1, c, range(4))
            build(late, c, range(4))
        return 0

    def sweep(xb, i):
        p = 16 + 4 * i
        for pair in range(2):
            add(xb, pair, sum(work(p + k, xb, pair) for k in range(4)))

    def phase_b1(i, _):
        @pl.when(i < 3)
        def _():
            for k in range(4):
                w.got_partner(20 + 4 * i + k)

        sweep(3, i)
        for k in range(4):
            for c in range(2):
                build(16 + lax.rem(4 * i + 4 + k, 16), c, range(4))
        return 0

    def ysend(label, d, slot, pair):
        tiles = pl.ds(2 * pair, 2)
        return lambda: pltpu.make_async_remote_copy(
            src_ref=yt.at[label, tiles], dst_ref=yin.at[slot, tiles], send_sem=ysem.at[0, slot, pair],
            recv_sem=ysem.at[1, slot, pair], device_id=xdev(d), device_id_type=MESH)

    sends = [[ysend(*who, pair) for pair in range(2)] for who in ((3, 2, 2), (2, 1, 0), (1, -1, 1))]

    def phase_b2(i, _):
        for n in range(3):
            for pair in range(2):
                pl.when(i == 4 * n + pair)(lambda n=n, pair=pair: sends[n][pair]().start())
        sweep(2 - lax.div(i, 4), lax.rem(i, 4))
        return 0

    for p in range(2):
        w.got_partner(p)
        for c in range(2):
            build(p, c, range(4))
    lax.fori_loop(0, 8, phase_0, 0)
    lax.fori_loop(0, 14, phase_a4, 0)
    lax.fori_loop(0, 4, phase_b1, 0)
    lax.fori_loop(0, 12, phase_b2, 0)
    for pairs in sends:
        for cp in pairs:
            cp().wait()
    for wait in w.sent:
        wait()
    for t in range(4):
        out_ref[t] = yt[0, t] + yin[0, t] + yin[1, t] + yin[2, t]


def solution(mesh):
    grid = Mesh(mesh.devices.reshape(2, 4, 4, 4), ('c', 'z', 'y', 'x'))
    spec = P(('z', 'y', 'x', 'c'), None)

    def per_device(x, v, ell, scale):
        anym, smem = pl.BlockSpec(memory_space=pl.ANY), pl.BlockSpec(memory_space=pltpu.SMEM)
        yt = pl.pallas_call(
            kernel,
            out_shape=jax.ShapeDtypeStruct((4, 128, TILE), F32),
            name='comm',
            in_specs=[smem, smem, anym, anym],
            out_specs=pl.BlockSpec(memory_space=pltpu.VMEM),
            scratch_shapes=[
                pltpu.VMEM((NPOS, 2, ROWS, 128), BF16),
                pltpu.VMEM((NPOS, 2, HALF, 128), BF16),
                pltpu.VMEM((4, 4, 2, TILE, 128), BF16),
                pltpu.VMEM((4, 4, 128, TILE), F32),
                pltpu.VMEM((3, 4, 128, TILE), F32),
                pltpu.VMEM((BLK, 128), BF16),
                pltpu.SemaphoreType.DMA((3,)),
                pltpu.SemaphoreType.DMA((100,)),
                pltpu.SemaphoreType.DMA((NPOS, 2)),
                pltpu.SemaphoreType.DMA((NPOS,)),
                pltpu.SemaphoreType.DMA((6,)),
                pltpu.SemaphoreType.DMA((2, 3, 2)),
            ],
            compiler_params=pltpu.CompilerParams(vmem_limit_bytes=60 * 2 ** 20, collective_id=0, has_side_effects=True),
        )(ell, scale, x, v)
        return yt.transpose(0, 2, 1).reshape(BLK, 128) * jnp.where(scale[0] < 0, -1.0, 1.0)

    return jax.shard_map(per_device, mesh=grid, in_specs=(spec, spec, P(None), P(None)), out_specs=spec, check_vma=False)
```

```python
import functools

import jax
import jax.numpy as jnp
from jax import lax
from jax.experimental import pallas as pl
from jax.experimental.pallas import tpu as pltpu
from jax.sharding import Mesh, PartitionSpec as P

F32 = jnp.float32
BF16 = jnp.bfloat16
MESH = pl.DeviceIdType.MESH
BLK = 1024
TILE = 256
HALF = 512
AUG0 = 2 * HALF
ROWS = AUG0 + 4 * 8
XROWS = 144
BF16_MAX = 3.3895313892515355e38
CORES = ((0,), (1,))
AHEAD = True

A, B = 0, 1
ORDER = [(0, 0, A), (0, 0, B),
         (0, -1, A), (0, 1, A), (-1, 0, B), (1, 0, B),
         (0, -1, B), (0, 1, B), (-1, 0, A), (1, 0, A),
         (-1, -1, B), (-1, 1, B), (-1, -1, A), (1, -1, A),
         (1, -1, B), (1, 1, B), (-1, 1, A), (1, 1, A),
         (0, 2, A), (2, 0, B), (0, 2, B), (2, 0, A),
         (2, -1, B), (2, 1, B), (-1, 2, A), (1, 2, A),
         (-1, 2, B), (1, 2, B), (2, -1, A), (2, 1, A),
         (2, 2, B), (2, 2, A)]
POS = {key: i for i, key in enumerate(ORDER)}
NPOS = len(ORDER)


def wrap(d):
    return (d + 1) % 4 - 1


def split3(n):
    hi = jnp.minimum(n, BF16_MAX).astype(BF16).astype(F32)
    r = n - hi
    mid = r.astype(BF16).astype(F32)
    return hi, mid, r - mid


class Wires:
    def __init__(self, cols, send, ici, d2d, pos):
        self.cols, self.send, self.ici, self.d2d, self.pos = cols, send, ici, d2d, pos
        self.sent = []
        self.dev = {(a, d): {a: lax.rem(pos[a] + d + 4, 4)} for a in 'zyx' for d in (1, -1, 2)}
        self.mate = {'c': 1 - pos['c']}

    def _copy(self, src, dst, recv, dev):
        n = len(self.sent)
        self.sent.append(lambda: pltpu.make_async_copy(src(), src(), self.send.at[n]).wait())
        pltpu.make_async_remote_copy(src_ref=src(), dst_ref=dst(), send_sem=self.send.at[n], recv_sem=recv(),
                                     device_id=dev, device_id_type=MESH).start()

    def block(self, key, c=0, part=None):
        p = POS[key]
        if part is None:
            return lambda: self.cols.at[p, c]
        return lambda: self.cols.at[p, c, pl.ds(part * (ROWS // 2), ROWS // 2)]

    def sem(self, key, part=0):
        return lambda: self.ici.at[POS[key], part]

    def both(self, axis, key):
        for sign in (1, -1):
            dz, dy, h = key
            dst = (dz, wrap(dy - sign), h) if axis == 'y' else (wrap(dz - sign), dy, h)
            self._copy(self.block(key), self.block(dst), self.sem(dst), self.dev[axis, sign])

    def relay(self, axis, off, h):
        dst = (off, 2, h) if axis == 'y' else (2, off, h)
        for part, sign in ((0, 1), (1, -1)):
            src = (off, -sign, h) if axis == 'y' else (-sign, off, h)
            self._copy(self.block(src, 0, part), self.block(dst, 0, part), self.sem(dst, part), self.dev[axis, sign])

    def partner(self, key):
        self._copy(self.block(key, 0), self.block(key, 1), lambda: self.d2d.at[POS[key]], self.mate)

    def _recv(self, dst, sem):
        pltpu.make_async_copy(dst, dst, sem).wait()

    def got(self, key):
        for part in (0, 1) if self.halved(key) else (None,):
            self._recv(self.block(key, 0, part)(), self.sem(key, part or 0)())

    @staticmethod
    def halved(key):
        dz, dy, h = key
        last = (dz if dz != 0 else dy) if h == A else (dy if dy != 0 else dz)
        return last == 2

    def got_partner(self, p):
        self._recv(self.cols.at[p, 1], self.d2d.at[p])


def schedule(w):
    def slot1():
        for key in [(0, -1, A), (0, 1, A), (-1, 0, B), (1, 0, B)]:
            w.got(key)
            w.partner(key)
        for d in (-1, 1):
            w.both('y', (d, 0, B))
            w.both('z', (0, d, A))
        w.relay('y', 0, A)
        w.relay('z', 0, B)

    def slot2():
        for key in [(0, -1, B), (0, 1, B), (-1, 0, A), (1, 0, A)]:
            w.got(key)
            w.partner(key)
        w.relay('y', 0, B)
        w.relay('z', 0, A)

    def slot3():
        for key in [(-1, -1, B), (-1, 1, B), (-1, -1, A), (1, -1, A)]:
            w.got(key)
            w.partner(key)

    def slot4():
        for key in [(0, 2, A), (2, 0, B)]:
            w.got(key)
            w.partner(key)
        w.both('y', (2, 0, B))
        w.both('z', (0, 2, A))
        for key in [(1, -1, B), (1, 1, B), (-1, 1, A), (1, 1, A)]:
            w.got(key)
            w.partner(key)
        for d in (-1, 1):
            w.relay('y', d, B)
            w.relay('z', d, A)

    def slot5():
        for key in [(0, 2, B), (2, 0, A)]:
            w.got(key)
            w.partner(key)

    def slot6():
        for key in [(2, -1, B), (2, 1, B), (-1, 2, A), (1, 2, A)]:
            w.got(key)
            w.partner(key)
        w.relay('y', 2, B)
        w.relay('z', 2, A)

    def slot7():
        for key in [(-1, 2, B), (1, 2, B), (2, -1, A), (2, 1, A)]:
            w.got(key)
            w.partner(key)

    def slot8():
        for key in [(2, 2, B), (2, 2, A)]:
            w.got(key)
            w.partner(key)

    return {1: slot1, 4: slot2, 8: slot3, 9: slot4, 10: slot5, 12: slot6, 14: slot7, 15: slot8}


def kernel(ell_ref, scale_ref, x_ref, v_ref, out_ref, cols, ag, xr, yt, yin, vbuf, local, send, ici, d2d, xsem, ysem):
    pos = {k: lax.axis_index(k) for k in ('c', 'z', 'y', 'x')}
    w = Wires(cols, send, ici, d2d, pos)
    xdev = lambda d: w.dev['x', d]

    loads = [pltpu.make_async_copy(x_ref.at[pl.ds(h * HALF, HALF)], cols.at[h, 0, pl.ds(0, HALF)], local.at[h]) for h in range(2)]
    loads.append(pltpu.make_async_copy(v_ref, vbuf, local.at[2]))
    for cp in loads:
        cp.start()
    barrier = pltpu.get_barrier_semaphore()
    peers = [w.dev[a, d] for a in 'zy' for d in (1, -1)] + [xdev(1), xdev(-1), xdev(2), w.mate]
    for dev in peers:
        pl.semaphore_signal(barrier, inc=1, device_id=dev, device_id_type=MESH)
    xr[:, :, :, pl.ds(XROWS, TILE - XROWS), :] = jnp.zeros((4, 4, 2, TILE - XROWS, 128), BF16)
    yt[...] = jnp.zeros_like(yt)

    ell = jnp.full((8, 128), ell_ref[0], F32)
    size = jnp.abs(jnp.full((8, 128), scale_ref[0], F32))
    two_ell_sq = 2.0 * ell * ell
    unit = jnp.exp2(jnp.clip(-jnp.ceil(jnp.log2(two_ell_sq)), -126.0, 40.0)).astype(BF16).astype(F32)
    unit = jnp.where(two_ell_sq > 3.4028234e38, 0.0, unit)
    factor = jnp.where(unit > 0.0, -1.4426950408889634 / (unit * two_ell_sq), -1.0)
    shift = jnp.maximum(jnp.log2(size), -400.0) / factor
    negc, cap = factor[0, 0], size[0, 0]
    unit, shift = unit[:1], shift[:1]

    for cp in loads:
        cp.wait()
    for t in range(8):
        half, at = t // 4, (t % 4) * 128
        xt = cols[half, 0, pl.ds(at, 128), :].astype(F32).T
        norm = jnp.sum(xt * xt, axis=0, keepdims=True)
        hi, mid, lo = split3(norm)
        row = lax.broadcasted_iota(jnp.int32, (16, 128), 0)
        ones = jnp.where(row < 6, 1.0, 0.0)
        left = jnp.where(row == 0, hi, jnp.where(row == 1, mid, jnp.where(row == 2, lo, ones)))
        hi, mid, lo = split3(norm * unit + shift)
        right = jnp.where(row == 3, hi, jnp.where(row == 4, mid, jnp.where(row == 5, lo, ones * unit)))
        cols[half, 0, pl.ds(AUG0 + (t % 4) * 8, 8), :] = left[:8].astype(BF16)
        xr[0, t // 2, t % 2, pl.ds(0, 128), :] = (xt * (-2.0 * unit)).astype(BF16)
        xr[0, t // 2, t % 2, pl.ds(128, 16), :] = right.astype(BF16)
        cols[half, 0, pl.ds(HALF + at, 128), :] = vbuf[pl.ds(t * 128, 128), :].astype(F32).T.astype(BF16)
    pl.semaphore_wait(barrier, len(peers))

    def xcopy(src, dst, tiles, recv, d):
        cut = lambda b: lambda: xr.at[b, pl.ds(*tiles), :, pl.ds(0, XROWS)]
        w._copy(cut(src), cut(dst), lambda: xsem.at[recv], xdev(d))

    def xgot(dst, tiles, recv):
        ref = xr.at[dst, pl.ds(*tiles), :, pl.ds(0, XROWS)]
        pltpu.make_async_copy(ref, ref, xsem.at[recv]).wait()

    w.partner((0, 0, A))
    w.partner((0, 0, B))
    for part in range(2):
        xcopy(0, 1, (2 * part, 2), part, 1)
        xcopy(0, 2, (2 * part, 2), 2 + part, -1)
    w.both('y', (0, 0, A))
    w.both('z', (0, 0, B))
    w.both('y', (0, 0, B))
    w.both('z', (0, 0, A))

    def build(p, c, tiles):
        for lt in tiles:
            piece = cols[p, c, pl.ds(AUG0 + lt * 8, 8), :].astype(F32)
            full = jnp.concatenate([piece, jnp.zeros((120, 128), F32)], axis=0)
            ag[p, c, pl.ds(lt * 128, 128), :] = full.T.astype(BF16)

    def gram(p, xb, pair, cores):
        lhs = jnp.concatenate([jnp.concatenate([cols[p, c, pl.ds(0, HALF), :], ag[p, c]], axis=1) for c in cores], axis=0)
        rhs = jnp.concatenate([jnp.concatenate([xr[xb, pair * 2 + q, h] for h in range(2)], axis=1) for q in range(2)], axis=1)
        return jnp.dot(lhs, rhs, preferred_element_type=F32)

    def apply(p, dist, cores):
        kern = jnp.exp2(dist * negc).astype(BF16)
        kern = jnp.minimum(kern, jnp.full(kern.shape, cap, F32).astype(BF16))
        vt = jnp.concatenate([cols[p, c, pl.ds(HALF + 128 * k, 128), :] for c in cores for k in range(4)], axis=1)
        return jnp.dot(vt, kern, preferred_element_type=F32)

    def group(work):
        todo = [(p, xb, pair, cores, i) for i, (ps, xb, pair) in enumerate(work) for p in ps for cores in CORES]
        sums = [None] * len(work)
        dist = gram(*todo[0][:4])
        for n, (p, xb, pair, cores, i) in enumerate(todo):
            now = dist
            if n + 1 < len(todo) and AHEAD:
                dist = gram(*todo[n + 1][:4])
            r = apply(p, now, cores)
            if n + 1 < len(todo) and not AHEAD:
                dist = gram(*todo[n + 1][:4])
            sums[i] = r if sums[i] is None else sums[i] + r
            if n + 1 == len(todo) or todo[n + 1][4] != i:
                for q in range(2):
                    yt[xb, pair * 2 + q] += sums[i][:, q * TILE:(q + 1) * TILE]

    acts = schedule(w)

    def phase_0(k, _):
        @pl.when(k == 2)
        def _():
            xgot(1, (0, 2), 0)

        @pl.when(k == 3)
        def _():
            xgot(2, (0, 2), 2)
            xcopy(1, 3, (0, 2), 4, 1)

        @pl.when(k == 4)
        def _():
            xgot(1, (2, 2), 1)

        @pl.when(k == 5)
        def _():
            xgot(2, (2, 2), 3)
            xcopy(2, 3, (2, 2), 5, -1)
            acts[1]()

        @pl.when(k == 6)
        def _():
            xgot(3, (0, 2), 4)

        @pl.when(k == 7)
        def _():
            xgot(3, (2, 2), 5)
            w.got_partner(2)

        a, b = lax.div(k, 2), lax.rem(k, 2)
        e = lax.div(a + 1, 2)
        inner = lax.rem(e, 2)
        xb = inner * (1 + b) + (1 - inner) * 3 * lax.div(e, 2)
        pair = inner * (a - 1) + (1 - inner) * b
        group([((0, 1), xb, pair)])
        for c in range(2):
            build(1 + lax.div(k, 7), c, range(4))
        return 0

    def phase_a4(n, _):
        p = n + 2
        for at, act in acts.items():
            if at > 1:
                pl.when(p == at)(act)
        w.got_partner(p + 1)
        late = p + lax.div(p, 12) * (5 - 3 * lax.div(p, 15))
        pl.when((p >= 12) & (p < 15))(lambda: w.got_partner(p + 5))
        group([((p,), xb, pair) for xb in range(4) for pair in range(2)])
        for c in range(2):
            build(p + 1, c, range(4))
            build(late, c, range(4))
        return 0

    def sweep(xb, i):
        p = 16 + 4 * i
        group([([p + k for k in range(4)], xb, pair) for pair in range(2)])

    def phase_b1(i, _):
        @pl.when(i < 3)
        def _():
            for k in range(4):
                w.got_partner(20 + 4 * i + k)

        sweep(3, i)
        for k in range(4):
            for c in range(2):
                build(16 + lax.rem(4 * i + 4 + k, 16), c, range(4))
        return 0

    def ysend(label, d, slot, pair):
        tiles = pl.ds(2 * pair, 2)
        return lambda: pltpu.make_async_remote_copy(
            src_ref=yt.at[label, tiles], dst_ref=yin.at[slot, tiles], send_sem=ysem.at[0, slot, pair],
            recv_sem=ysem.at[1, slot, pair], device_id=xdev(d), device_id_type=MESH)

    sends = [[ysend(*who, pair) for pair in range(2)] for who in ((3, 2, 2), (2, 1, 0), (1, -1, 1))]

    def phase_b2(i, _):
        for n in range(3):
            for pair in range(2):
                pl.when(i == 4 * n + pair)(lambda n=n, pair=pair: sends[n][pair]().start())
        sweep(2 - lax.div(i, 4), lax.rem(i, 4))
        return 0

    for p in range(2):
        w.got_partner(p)
        for c in range(2):
            build(p, c, range(4))
    lax.fori_loop(0, 8, phase_0, 0)
    lax.fori_loop(0, 14, phase_a4, 0)
    lax.fori_loop(0, 4, phase_b1, 0)
    lax.fori_loop(0, 12, phase_b2, 0)
    for pairs in sends:
        for cp in pairs:
            cp().wait()
    for wait in w.sent:
        wait()
    for t in range(4):
        out_ref[t] = yt[0, t] + yin[0, t] + yin[1, t] + yin[2, t]


def solution(mesh):
    grid = Mesh(mesh.devices.reshape(2, 4, 4, 4), ('c', 'z', 'y', 'x'))
    spec = P(('z', 'y', 'x', 'c'), None)

    def per_device(x, v, ell, scale):
        anym, smem = pl.BlockSpec(memory_space=pl.ANY), pl.BlockSpec(memory_space=pltpu.SMEM)
        yt = pl.pallas_call(
            kernel,
            out_shape=jax.ShapeDtypeStruct((4, 128, TILE), F32),
            name='comm',
            in_specs=[smem, smem, anym, anym],
            out_specs=pl.BlockSpec(memory_space=pltpu.VMEM),
            scratch_shapes=[
                pltpu.VMEM((NPOS, 2, ROWS, 128), BF16),
                pltpu.VMEM((NPOS, 2, HALF, 128), BF16),
                pltpu.VMEM((4, 4, 2, TILE, 128), BF16),
                pltpu.VMEM((4, 4, 128, TILE), F32),
                pltpu.VMEM((3, 4, 128, TILE), F32),
                pltpu.VMEM((BLK, 128), BF16),
                pltpu.SemaphoreType.DMA((3,)),
                pltpu.SemaphoreType.DMA((100,)),
                pltpu.SemaphoreType.DMA((NPOS, 2)),
                pltpu.SemaphoreType.DMA((NPOS,)),
                pltpu.SemaphoreType.DMA((6,)),
                pltpu.SemaphoreType.DMA((2, 3, 2)),
            ],
            compiler_params=pltpu.CompilerParams(vmem_limit_bytes=60 * 2 ** 20, collective_id=0, has_side_effects=True),
        )(ell, scale, x, v)
        return yt.transpose(0, 2, 1).reshape(BLK, 128) * jnp.where(scale[0] < 0, -1.0, 1.0)

    return jax.shard_map(per_device, mesh=grid, in_specs=(spec, spec, P(None), P(None)), out_specs=spec, check_vma=False)
```

```python
import functools

import jax
import jax.numpy as jnp
from jax import lax
from jax.experimental import pallas as pl
from jax.experimental.pallas import tpu as pltpu
from jax.sharding import Mesh, PartitionSpec as P

F32 = jnp.float32
BF16 = jnp.bfloat16
MESH = pl.DeviceIdType.MESH
BLK = 1024
TILE = 256
HALF = 512
AUG0 = 2 * HALF
ROWS = AUG0 + 4 * 8
XROWS = 144
BF16_MAX = 3.3895313892515355e38
CORES = ((0,), (1,))
AHEAD = True

A, B = 0, 1
ORDER = [(0, 0, A), (0, 0, B),
         (0, -1, A), (0, 1, A), (-1, 0, B), (1, 0, B),
         (0, -1, B), (0, 1, B), (-1, 0, A), (1, 0, A),
         (-1, -1, B), (-1, 1, B), (-1, -1, A), (1, -1, A),
         (1, -1, B), (1, 1, B), (-1, 1, A), (1, 1, A),
         (0, 2, A), (2, 0, B), (0, 2, B), (2, 0, A),
         (2, -1, B), (2, 1, B), (-1, 2, A), (1, 2, A),
         (-1, 2, B), (1, 2, B), (2, -1, A), (2, 1, A),
         (2, 2, B), (2, 2, A)]
POS = {key: i for i, key in enumerate(ORDER)}
NPOS = len(ORDER)


def wrap(d):
    return (d + 1) % 4 - 1


def split3(n):
    hi = jnp.minimum(n, BF16_MAX).astype(BF16).astype(F32)
    r = n - hi
    mid = r.astype(BF16).astype(F32)
    return hi, mid, r - mid


class Wires:
    def __init__(self, cols, send, ici, d2d, pos):
        self.cols, self.send, self.ici, self.d2d, self.pos = cols, send, ici, d2d, pos
        self.sent = []
        self.dev = {(a, d): {a: lax.rem(pos[a] + d + 4, 4)} for a in 'zyx' for d in (1, -1, 2)}
        self.mate = {'c': 1 - pos['c']}

    def _copy(self, src, dst, recv, dev):
        n = len(self.sent)
        self.sent.append(lambda: pltpu.make_async_copy(src(), src(), self.send.at[n]).wait())
        pltpu.make_async_remote_copy(src_ref=src(), dst_ref=dst(), send_sem=self.send.at[n], recv_sem=recv(),
                                     device_id=dev, device_id_type=MESH).start()

    def block(self, key, c=0, part=None):
        p = POS[key]
        if part is None:
            return lambda: self.cols.at[p, c]
        return lambda: self.cols.at[p, c, pl.ds(part * (ROWS // 2), ROWS // 2)]

    def sem(self, key, part=0):
        return lambda: self.ici.at[POS[key], part]

    def both(self, axis, key):
        for sign in (1, -1):
            dz, dy, h = key
            dst = (dz, wrap(dy - sign), h) if axis == 'y' else (wrap(dz - sign), dy, h)
            self._copy(self.block(key), self.block(dst), self.sem(dst), self.dev[axis, sign])

    def relay(self, axis, off, h):
        dst = (off, 2, h) if axis == 'y' else (2, off, h)
        for part, sign in ((0, 1), (1, -1)):
            src = (off, -sign, h) if axis == 'y' else (-sign, off, h)
            self._copy(self.block(src, 0, part), self.block(dst, 0, part), self.sem(dst, part), self.dev[axis, sign])

    def partner(self, key):
        self._copy(self.block(key, 0), self.block(key, 1), lambda: self.d2d.at[POS[key]], self.mate)

    def _recv(self, dst, sem):
        pltpu.make_async_copy(dst, dst, sem).wait()

    def got(self, key):
        for part in (0, 1) if self.halved(key) else (None,):
            self._recv(self.block(key, 0, part)(), self.sem(key, part or 0)())

    @staticmethod
    def halved(key):
        dz, dy, h = key
        last = (dz if dz != 0 else dy) if h == A else (dy if dy != 0 else dz)
        return last == 2

    def got_partner(self, p):
        self._recv(self.cols.at[p, 1], self.d2d.at[p])


def schedule(w):
    def slot1():
        for key in [(0, -1, A), (0, 1, A), (-1, 0, B), (1, 0, B)]:
            w.got(key)
            w.partner(key)
        for d in (-1, 1):
            w.both('y', (d, 0, B))
            w.both('z', (0, d, A))
        w.relay('y', 0, A)
        w.relay('z', 0, B)

    def slot2():
        for key in [(0, -1, B), (0, 1, B), (-1, 0, A), (1, 0, A)]:
            w.got(key)
            w.partner(key)
        w.relay('y', 0, B)
        w.relay('z', 0, A)

    def slot3():
        for key in [(-1, -1, B), (-1, 1, B), (-1, -1, A), (1, -1, A)]:
            w.got(key)
            w.partner(key)

    def slot4():
        for key in [(0, 2, A), (2, 0, B)]:
            w.got(key)
            w.partner(key)
        w.both('y', (2, 0, B))
        w.both('z', (0, 2, A))
        for key in [(1, -1, B), (1, 1, B), (-1, 1, A), (1, 1, A)]:
            w.got(key)
            w.partner(key)
        for d in (-1, 1):
            w.relay('y', d, B)
            w.relay('z', d, A)

    def slot5():
        for key in [(0, 2, B), (2, 0, A)]:
            w.got(key)
            w.partner(key)

    def slot6():
        for key in [(2, -1, B), (2, 1, B), (-1, 2, A), (1, 2, A)]:
            w.got(key)
            w.partner(key)
        w.relay('y', 2, B)
        w.relay('z', 2, A)

    def slot7():
        for key in [(-1, 2, B), (1, 2, B), (2, -1, A), (2, 1, A)]:
            w.got(key)
            w.partner(key)

    def slot8():
        for key in [(2, 2, B), (2, 2, A)]:
            w.got(key)
            w.partner(key)

    return {1: slot1, 4: slot2, 8: slot3, 9: slot4, 10: slot5, 12: slot6, 14: slot7, 15: slot8}


def kernel(ell_ref, scale_ref, x_ref, v_ref, out_ref, cols, ag, xr, yt, yin, vbuf, local, send, ici, d2d, xsem, ysem):
    pos = {k: lax.axis_index(k) for k in ('c', 'z', 'y', 'x')}
    w = Wires(cols, send, ici, d2d, pos)
    xdev = lambda d: w.dev['x', d]

    loads = [pltpu.make_async_copy(x_ref.at[pl.ds(h * HALF, HALF)], cols.at[h, 0, pl.ds(0, HALF)], local.at[h]) for h in range(2)]
    loads.append(pltpu.make_async_copy(v_ref, vbuf, local.at[2]))
    for cp in loads:
        cp.start()
    barrier = pltpu.get_barrier_semaphore()
    peers = [w.dev[a, d] for a in 'zy' for d in (1, -1)] + [xdev(1), xdev(-1), xdev(2), w.mate]
    for dev in peers:
        pl.semaphore_signal(barrier, inc=1, device_id=dev, device_id_type=MESH)
    xr[:, :, :, pl.ds(XROWS, TILE - XROWS), :] = jnp.zeros((4, 4, 2, TILE - XROWS, 128), BF16)
    yt[...] = jnp.zeros_like(yt)

    ell = jnp.full((8, 128), ell_ref[0], F32)
    size = jnp.abs(jnp.full((8, 128), scale_ref[0], F32))
    two_ell_sq = 2.0 * ell * ell
    unit = jnp.exp2(jnp.clip(-jnp.ceil(jnp.log2(two_ell_sq)), -126.0, 40.0)).astype(BF16).astype(F32)
    unit = jnp.where(two_ell_sq > 3.4028234e38, 0.0, unit)
    factor = jnp.where(unit > 0.0, -1.4426950408889634 / (unit * two_ell_sq), -1.0)
    shift = jnp.maximum(jnp.log2(size), -400.0) / factor
    negc, cap = factor[0, 0], size[0, 0]
    sign = jnp.where(jnp.full((8, 128), scale_ref[0], F32) < 0.0, -1.0, 1.0)[0, 0]
    unit, shift = unit[:1], shift[:1]

    for cp in loads:
        cp.wait()
    for t in range(8):
        half, at = t // 4, (t % 4) * 128
        xt = cols[half, 0, pl.ds(at, 128), :].astype(F32).T
        norm = jnp.sum(xt * xt, axis=0, keepdims=True)
        hi, mid, lo = split3(norm)
        row = lax.broadcasted_iota(jnp.int32, (16, 128), 0)
        ones = jnp.where(row < 6, 1.0, 0.0)
        left = jnp.where(row == 0, hi, jnp.where(row == 1, mid, jnp.where(row == 2, lo, ones)))
        hi, mid, lo = split3(norm * unit + shift)
        right = jnp.where(row == 3, hi, jnp.where(row == 4, mid, jnp.where(row == 5, lo, ones * unit)))
        cols[half, 0, pl.ds(AUG0 + (t % 4) * 8, 8), :] = left[:8].astype(BF16)
        xr[0, t // 2, t % 2, pl.ds(0, 128), :] = (xt * (-2.0 * unit)).astype(BF16)
        xr[0, t // 2, t % 2, pl.ds(128, 16), :] = right.astype(BF16)
        cols[half, 0, pl.ds(HALF + at, 128), :] = vbuf[pl.ds(t * 128, 128), :].astype(F32).T.astype(BF16)
    pl.semaphore_wait(barrier, len(peers))

    def xcopy(src, dst, tiles, recv, d):
        cut = lambda b: lambda: xr.at[b, pl.ds(*tiles), :, pl.ds(0, XROWS)]
        w._copy(cut(src), cut(dst), lambda: xsem.at[recv], xdev(d))

    def xgot(dst, tiles, recv):
        ref = xr.at[dst, pl.ds(*tiles), :, pl.ds(0, XROWS)]
        pltpu.make_async_copy(ref, ref, xsem.at[recv]).wait()

    w.partner((0, 0, A))
    w.partner((0, 0, B))
    for part in range(2):
        xcopy(0, 1, (2 * part, 2), part, 1)
        xcopy(0, 2, (2 * part, 2), 2 + part, -1)
    w.both('y', (0, 0, A))
    w.both('z', (0, 0, B))
    w.both('y', (0, 0, B))
    w.both('z', (0, 0, A))

    def build(p, c, tiles):
        for lt in tiles:
            piece = cols[p, c, pl.ds(AUG0 + lt * 8, 8), :].astype(F32)
            full = jnp.concatenate([piece, jnp.zeros((120, 128), F32)], axis=0)
            ag[p, c, pl.ds(lt * 128, 128), :] = full.T.astype(BF16)

    def gram(p, xb, pair, cores):
        lhs = jnp.concatenate([jnp.concatenate([cols[p, c, pl.ds(0, HALF), :], ag[p, c]], axis=1) for c in cores], axis=0)
        rhs = jnp.concatenate([jnp.concatenate([xr[xb, pair * 2 + q, h] for h in range(2)], axis=1) for q in range(2)], axis=1)
        return jnp.dot(lhs, rhs, preferred_element_type=F32)

    def apply(p, dist, cores):
        kern = jnp.exp2(dist * negc).astype(BF16)
        kern = jnp.minimum(kern, jnp.full(kern.shape, cap, F32).astype(BF16))
        vt = jnp.concatenate([cols[p, c, pl.ds(HALF + 128 * k, 128), :] for c in cores for k in range(4)], axis=1)
        return jnp.dot(vt, kern, preferred_element_type=F32)

    def group(work):
        todo = [(p, xb, pair, cores, i) for i, (ps, xb, pair) in enumerate(work) for p in ps for cores in CORES]
        sums = [None] * len(work)
        dist = gram(*todo[0][:4])
        for n, (p, xb, pair, cores, i) in enumerate(todo):
            now = dist
            if n + 1 < len(todo) and AHEAD:
                dist = gram(*todo[n + 1][:4])
            r = apply(p, now, cores)
            if n + 1 < len(todo) and not AHEAD:
                dist = gram(*todo[n + 1][:4])
            sums[i] = r if sums[i] is None else sums[i] + r
            if n + 1 == len(todo) or todo[n + 1][4] != i:
                for q in range(2):
                    yt[xb, pair * 2 + q] += sums[i][:, q * TILE:(q + 1) * TILE]

    acts = schedule(w)

    def phase_0(k, _):
        @pl.when(k == 2)
        def _():
            xgot(1, (0, 2), 0)

        @pl.when(k == 3)
        def _():
            xgot(2, (0, 2), 2)
            xcopy(1, 3, (0, 2), 4, 1)

        @pl.when(k == 4)
        def _():
            xgot(1, (2, 2), 1)
            xgot(2, (2, 2), 3)
            xcopy(2, 3, (2, 2), 5, -1)

        @pl.when(k == 5)
        def _():
            acts[1]()

        @pl.when(k == 6)
        def _():
            for p in (2, 3):
                w.got_partner(p)
                for c in range(2):
                    build(p, c, range(4))

        @pl.when(k == 7)
        def _():
            w.got_partner(4)

        p, n = 2 * lax.div(k, 6), lax.rem(k, 6)
        a, b = lax.div(n, 2), lax.rem(n, 2)
        inner = lax.div(a + 1, 2)
        group([((p, p + 1), inner * (1 + b), inner * (a - 1) + (1 - inner) * b)])
        for c in range(2):
            build(1 + 3 * lax.div(k, 7), c, range(4))
        return 0

    def phase_a4(n, _):
        p = n + 4

        @pl.when(p == 4)
        def _():
            xgot(3, (0, 2), 4)
            xgot(3, (2, 2), 5)

        for at, act in acts.items():
            if at > 1:
                pl.when(p == at)(act)
        w.got_partner(p + 1)
        late = p + lax.div(p, 12) * (5 - 3 * lax.div(p, 15))
        pl.when((p >= 12) & (p < 15))(lambda: w.got_partner(p + 5))
        group([((p,), xb, pair) for xb in range(4) for pair in range(2)])
        for c in range(2):
            build(p + 1, c, range(4))
            build(late, c, range(4))
        return 0

    def sweep(xb, i):
        p = lax.rem(16 + 4 * i, 32)
        group([([p + k for k in range(4)], xb, pair) for pair in range(2)])

    def phase_b1(i, _):
        @pl.when(i < 3)
        def _():
            for k in range(4):
                w.got_partner(20 + 4 * i + k)

        sweep(3, i)
        for k in range(4):
            for c in range(2):
                build(16 + lax.rem(4 * i + 4 + k, 16), c, range(4))
        return 0

    def ysend(label, d, slot, pair):
        tiles = pl.ds(2 * pair, 2)
        return lambda: pltpu.make_async_remote_copy(
            src_ref=yt.at[label, tiles], dst_ref=yin.at[slot, tiles], send_sem=ysem.at[0, slot, pair],
            recv_sem=ysem.at[1, slot, pair], device_id=xdev(d), device_id_type=MESH)

    sends = [[ysend(*who, pair) for pair in range(2)] for who in ((3, 2, 2), (2, 1, 0), (1, -1, 1))]

    def phase_b2(i, _):
        for n in range(3):
            for pair in range(2):
                pl.when(i == 4 * n + pair)(lambda n=n, pair=pair: sends[n][pair]().start())
        sweep(2 - lax.div(i, 4), lax.rem(i, 4))
        return 0

    for p in range(2):
        w.got_partner(p)
        for c in range(2):
            build(p, c, range(4))
    lax.fori_loop(0, 12, phase_0, 0)
    lax.fori_loop(0, 12, phase_a4, 0)
    lax.fori_loop(0, 5, phase_b1, 0)
    lax.fori_loop(0, 12, phase_b2, 0)
    for pairs in sends:
        for cp in pairs:
            cp().wait()
    for wait in w.sent:
        wait()
    for t in range(4):
        out_ref[t] = (yt[0, t] + yin[0, t] + yin[1, t] + yin[2, t]) * sign


def solution(mesh):
    grid = Mesh(mesh.devices.reshape(2, 4, 4, 4), ('c', 'z', 'y', 'x'))
    spec = P(('z', 'y', 'x', 'c'), None)

    def per_device(x, v, ell, scale):
        anym, smem = pl.BlockSpec(memory_space=pl.ANY), pl.BlockSpec(memory_space=pltpu.SMEM)
        yt = pl.pallas_call(
            kernel,
            out_shape=jax.ShapeDtypeStruct((4, 128, TILE), F32),
            name='comm',
            in_specs=[smem, smem, anym, anym],
            out_specs=pl.BlockSpec(memory_space=pltpu.VMEM),
            scratch_shapes=[
                pltpu.VMEM((NPOS, 2, ROWS, 128), BF16),
                pltpu.VMEM((NPOS, 2, HALF, 128), BF16),
                pltpu.VMEM((4, 4, 2, TILE, 128), BF16),
                pltpu.VMEM((4, 4, 128, TILE), F32),
                pltpu.VMEM((3, 4, 128, TILE), F32),
                pltpu.VMEM((BLK, 128), BF16),
                pltpu.SemaphoreType.DMA((3,)),
                pltpu.SemaphoreType.DMA((100,)),
                pltpu.SemaphoreType.DMA((NPOS, 2)),
                pltpu.SemaphoreType.DMA((NPOS,)),
                pltpu.SemaphoreType.DMA((6,)),
                pltpu.SemaphoreType.DMA((2, 3, 2)),
            ],
            compiler_params=pltpu.CompilerParams(vmem_limit_bytes=60 * 2 ** 20, collective_id=0, has_side_effects=True),
        )(ell, scale, x, v)
        return yt.transpose(0, 2, 1).reshape(BLK, 128)

    return jax.shard_map(per_device, mesh=grid, in_specs=(spec, spec, P(None), P(None)), out_specs=spec, check_vma=False)
```

```python
import functools

import jax
import jax.numpy as jnp
from jax import lax
from jax.experimental import pallas as pl
from jax.experimental.pallas import tpu as pltpu
from jax.sharding import Mesh, PartitionSpec as P

F32 = jnp.float32
BF16 = jnp.bfloat16
MESH = pl.DeviceIdType.MESH
BLK = 1024
TILE = 256
HALF = 512
AUG0 = 2 * HALF
ROWS = AUG0 + 4 * 8
XROWS = 144
BF16_MAX = 3.3895313892515355e38

A, B = 0, 1
ORDER = [(0, 0, A), (0, 0, B),
         (0, -1, A), (0, 1, A), (-1, 0, B), (1, 0, B),
         (0, -1, B), (0, 1, B), (-1, 0, A), (1, 0, A),
         (-1, -1, B), (-1, 1, B), (-1, -1, A), (1, -1, A),
         (1, -1, B), (1, 1, B), (-1, 1, A), (1, 1, A),
         (0, 2, A), (2, 0, B), (0, 2, B), (2, 0, A),
         (2, -1, B), (2, 1, B), (-1, 2, A), (1, 2, A),
         (-1, 2, B), (1, 2, B), (2, -1, A), (2, 1, A),
         (2, 2, B), (2, 2, A)]
POS = {key: i for i, key in enumerate(ORDER)}
NPOS = len(ORDER)


def wrap(d):
    return (d + 1) % 4 - 1


def split3(n):
    hi = jnp.minimum(n, BF16_MAX).astype(BF16).astype(F32)
    r = n - hi
    mid = r.astype(BF16).astype(F32)
    return hi, mid, r - mid


class Wires:
    def __init__(self, cols, send, ici, d2d, pos):
        self.cols, self.send, self.ici, self.d2d, self.pos = cols, send, ici, d2d, pos
        self.sent = []
        self.dev = {(a, d): {a: lax.rem(pos[a] + d + 4, 4)} for a in 'zyx' for d in (1, -1, 2)}
        self.mate = {'c': 1 - pos['c']}

    def _copy(self, src, dst, recv, dev):
        n = len(self.sent)
        self.sent.append(lambda: pltpu.make_async_copy(src(), src(), self.send.at[n]).wait())
        pltpu.make_async_remote_copy(src_ref=src(), dst_ref=dst(), send_sem=self.send.at[n], recv_sem=recv(),
                                     device_id=dev, device_id_type=MESH).start()

    def block(self, key, c=0, part=None):
        p = POS[key]
        if part is None:
            return lambda: self.cols.at[p, c]
        return lambda: self.cols.at[p, c, pl.ds(part * (ROWS // 2), ROWS // 2)]

    def sem(self, key, part=0):
        return lambda: self.ici.at[POS[key], part]

    def both(self, axis, key):
        for sign in (1, -1):
            dz, dy, h = key
            dst = (dz, wrap(dy - sign), h) if axis == 'y' else (wrap(dz - sign), dy, h)
            self._copy(self.block(key), self.block(dst), self.sem(dst), self.dev[axis, sign])

    def relay(self, axis, off, h):
        dst = (off, 2, h) if axis == 'y' else (2, off, h)
        for part, sign in ((0, 1), (1, -1)):
            src = (off, -sign, h) if axis == 'y' else (-sign, off, h)
            self._copy(self.block(src, 0, part), self.block(dst, 0, part), self.sem(dst, part), self.dev[axis, sign])

    def partner(self, key):
        self._copy(self.block(key, 0), self.block(key, 1), lambda: self.d2d.at[POS[key]], self.mate)

    def _recv(self, dst, sem):
        pltpu.make_async_copy(dst, dst, sem).wait()

    def got(self, key):
        for part in (0, 1) if self.halved(key) else (None,):
            self._recv(self.block(key, 0, part)(), self.sem(key, part or 0)())

    @staticmethod
    def halved(key):
        dz, dy, h = key
        last = (dz if dz != 0 else dy) if h == A else (dy if dy != 0 else dz)
        return last == 2

    def got_partner(self, p):
        self._recv(self.cols.at[p, 1], self.d2d.at[p])


def schedule(w):
    def slot1():
        for key in [(0, -1, A), (0, 1, A), (-1, 0, B), (1, 0, B)]:
            w.got(key)
            w.partner(key)
        for d in (-1, 1):
            w.both('y', (d, 0, B))
            w.both('z', (0, d, A))
        w.relay('y', 0, A)
        w.relay('z', 0, B)

    def slot2():
        for key in [(0, -1, B), (0, 1, B), (-1, 0, A), (1, 0, A)]:
            w.got(key)
            w.partner(key)
        w.relay('y', 0, B)
        w.relay('z', 0, A)

    def slot3():
        for key in [(-1, -1, B), (-1, 1, B), (-1, -1, A), (1, -1, A)]:
            w.got(key)
            w.partner(key)

    def slot4():
        for key in [(0, 2, A), (2, 0, B)]:
            w.got(key)
            w.partner(key)
        w.both('y', (2, 0, B))
        w.both('z', (0, 2, A))
        for key in [(1, -1, B), (1, 1, B), (-1, 1, A), (1, 1, A)]:
            w.got(key)
            w.partner(key)
        for d in (-1, 1):
            w.relay('y', d, B)
            w.relay('z', d, A)

    def slot5():
        for key in [(0, 2, B), (2, 0, A)]:
            w.got(key)
            w.partner(key)

    def slot6():
        for key in [(2, -1, B), (2, 1, B), (-1, 2, A), (1, 2, A)]:
            w.got(key)
            w.partner(key)
        w.relay('y', 2, B)
        w.relay('z', 2, A)

    def slot7():
        for key in [(-1, 2, B), (1, 2, B), (2, -1, A), (2, 1, A)]:
            w.got(key)
            w.partner(key)

    def slot8():
        for key in [(2, 2, B), (2, 2, A)]:
            w.got(key)
            w.partner(key)

    return {1: slot1, 4: slot2, 8: slot3, 9: slot4, 10: slot5, 12: slot6, 14: slot7, 15: slot8}


def kernel(ell_ref, scale_ref, x_ref, v_ref, out_ref, cols, ag, xr, yt, yin, vbuf, local, send, ici, d2d, xsem, ysem):
    pos = {k: lax.axis_index(k) for k in ('c', 'z', 'y', 'x')}
    w = Wires(cols, send, ici, d2d, pos)
    xdev = lambda d: w.dev['x', d]

    loads = [pltpu.make_async_copy(x_ref.at[pl.ds(h * HALF, HALF)], cols.at[h, 0, pl.ds(0, HALF)], local.at[h]) for h in range(2)]
    loads.append(pltpu.make_async_copy(v_ref, vbuf, local.at[2]))
    for cp in loads:
        cp.start()
    barrier = pltpu.get_barrier_semaphore()
    peers = [w.dev[a, d] for a in 'zy' for d in (1, -1)] + [xdev(1), xdev(-1), xdev(2), w.mate]
    for dev in peers:
        pl.semaphore_signal(barrier, inc=1, device_id=dev, device_id_type=MESH)
    xr[:, :, :, pl.ds(XROWS, TILE - XROWS), :] = jnp.zeros((4, 4, 2, TILE - XROWS, 128), BF16)
    yt[...] = jnp.zeros_like(yt)

    ell = jnp.full((8, 128), ell_ref[0], F32)
    size = jnp.abs(jnp.full((8, 128), scale_ref[0], F32))
    two_ell_sq = 2.0 * ell * ell
    unit = jnp.exp2(jnp.clip(-jnp.ceil(jnp.log2(two_ell_sq)), -126.0, 40.0)).astype(BF16).astype(F32)
    unit = jnp.where(two_ell_sq > 3.4028234e38, 0.0, unit)
    factor = jnp.where(unit > 0.0, -1.4426950408889634 / (unit * two_ell_sq), -1.0)
    shift = jnp.maximum(jnp.log2(size), -400.0) / factor
    negc, cap = factor[0, 0], size[0, 0]
    sign = jnp.where(jnp.full((8, 128), scale_ref[0], F32) < 0.0, -1.0, 1.0)[0, 0]
    unit, shift = unit[:1], shift[:1]

    for cp in loads:
        cp.wait()
    for t in range(8):
        half, at = t // 4, (t % 4) * 128
        xt = cols[half, 0, pl.ds(at, 128), :].astype(F32).T
        norm = jnp.sum(xt * xt, axis=0, keepdims=True)
        hi, mid, lo = split3(norm)
        row = lax.broadcasted_iota(jnp.int32, (16, 128), 0)
        ones = jnp.where(row < 6, 1.0, 0.0)
        left = jnp.where(row == 0, hi, jnp.where(row == 1, mid, jnp.where(row == 2, lo, ones)))
        hi, mid, lo = split3(norm * unit + shift)
        right = jnp.where(row == 3, hi, jnp.where(row == 4, mid, jnp.where(row == 5, lo, ones * unit)))
        cols[half, 0, pl.ds(AUG0 + (t % 4) * 8, 8), :] = left[:8].astype(BF16)
        xr[0, t // 2, t % 2, pl.ds(0, 128), :] = (xt * (-2.0 * unit)).astype(BF16)
        xr[0, t // 2, t % 2, pl.ds(128, 16), :] = right.astype(BF16)
        cols[half, 0, pl.ds(HALF + at, 128), :] = vbuf[pl.ds(t * 128, 128), :].astype(F32).T.astype(BF16)
    pl.semaphore_wait(barrier, len(peers))

    def xcopy(src, dst, tiles, recv, d):
        cut = lambda b: lambda: xr.at[b, pl.ds(*tiles), :, pl.ds(0, XROWS)]
        w._copy(cut(src), cut(dst), lambda: xsem.at[recv], xdev(d))

    def xgot(dst, tiles, recv):
        ref = xr.at[dst, pl.ds(*tiles), :, pl.ds(0, XROWS)]
        pltpu.make_async_copy(ref, ref, xsem.at[recv]).wait()

    w.partner((0, 0, A))
    w.partner((0, 0, B))
    for part in range(2):
        xcopy(0, 1, (2 * part, 2), part, 1)
        xcopy(0, 2, (2 * part, 2), 2 + part, -1)
    w.both('y', (0, 0, A))
    w.both('z', (0, 0, B))
    w.both('y', (0, 0, B))
    w.both('z', (0, 0, A))

    def build(p, c, tiles):
        for lt in tiles:
            piece = cols[p, c, pl.ds(AUG0 + lt * 8, 8), :].astype(F32)
            full = jnp.concatenate([piece, jnp.zeros((120, 128), F32)], axis=0)
            ag[p, c, pl.ds(lt * 128, 128), :] = full.T.astype(BF16)

    def gram(p, xb, pair, cores):
        lhs = jnp.concatenate([jnp.concatenate([cols[p, c, pl.ds(0, HALF), :], ag[p, c]], axis=1) for c in cores], axis=0)
        rhs = jnp.concatenate([jnp.concatenate([xr[xb, pair * 2 + q, h] for h in range(2)], axis=1) for q in range(2)], axis=1)
        return jnp.dot(lhs, rhs, preferred_element_type=F32)

    def values(dist):
        kern = jnp.exp2(dist * negc).astype(BF16)
        return jnp.minimum(kern, jnp.full(kern.shape, cap, F32).astype(BF16))

    def product(p, xb, pair, cores, kern):
        vt = jnp.concatenate([cols[p, c, pl.ds(HALF + 128 * k, 128), :] for c in cores for k in range(4)], axis=1)
        r = jnp.dot(vt, kern, preferred_element_type=F32)
        for q in range(2):
            yt[xb, pair * 2 + q] += r[:, q * TILE:(q + 1) * TILE]

    def group(work):
        todo = [(p, xb, pair, cores) for ps, xb, pair in work for p in ps for cores in ((0,), (1,))]
        dist = gram(*todo[0])
        for n, (p, xb, pair, cores) in enumerate(todo):
            now = dist
            if n + 1 < len(todo):
                dist = gram(*todo[n + 1])
            product(p, xb, pair, cores, values(now))

    acts = schedule(w)

    def phase_0(k, _):
        @pl.when(k == 2)
        def _():
            xgot(1, (0, 2), 0)

        @pl.when(k == 3)
        def _():
            xgot(2, (0, 2), 2)
            xcopy(1, 3, (0, 2), 4, 1)

        @pl.when(k == 4)
        def _():
            xgot(1, (2, 2), 1)

        @pl.when(k == 5)
        def _():
            xgot(2, (2, 2), 3)
            xcopy(2, 3, (2, 2), 5, -1)
            acts[1]()

        @pl.when(k == 6)
        def _():
            xgot(3, (0, 2), 4)

        @pl.when(k == 7)
        def _():
            xgot(3, (2, 2), 5)
            w.got_partner(2)

        a, b = lax.div(k, 2), lax.rem(k, 2)
        e = lax.div(a + 1, 2)
        inner = lax.rem(e, 2)
        xb = inner * (1 + b) + (1 - inner) * 3 * lax.div(e, 2)
        pair = inner * (a - 1) + (1 - inner) * b
        group([((0, 1), xb, pair)])
        for c in range(2):
            build(1 + lax.div(k, 7), c, range(4))
        return 0

    def phase_a4(n, _):
        p = n + 2
        for at, act in acts.items():
            if at > 1:
                pl.when(p == at)(act)
        w.got_partner(p + 1)
        late = p + lax.div(p, 12) * (5 - 3 * lax.div(p, 15))
        pl.when((p >= 12) & (p < 15))(lambda: w.got_partner(p + 5))
        group([((p,), xb, pair) for xb in range(4) for pair in range(2)])
        for c in range(2):
            build(p + 1, c, range(4))
            build(late, c, range(4))
        return 0

    def sweep(xb, i):
        p = 16 + 4 * i
        group([([p + k for k in range(4)], xb, pair) for pair in range(2)])

    def phase_b1(i, _):
        @pl.when(i < 3)
        def _():
            for k in range(4):
                w.got_partner(20 + 4 * i + k)

        sweep(3, i)
        for k in range(4):
            for c in range(2):
                build(16 + lax.rem(4 * i + 4 + k, 16), c, range(4))
        return 0

    def ysend(label, d, slot, pair):
        tiles = pl.ds(2 * pair, 2)
        return lambda: pltpu.make_async_remote_copy(
            src_ref=yt.at[label, tiles], dst_ref=yin.at[slot, tiles], send_sem=ysem.at[0, slot, pair],
            recv_sem=ysem.at[1, slot, pair], device_id=xdev(d), device_id_type=MESH)

    sends = [[ysend(*who, pair) for pair in range(2)] for who in ((3, 2, 2), (2, 1, 0), (1, -1, 1))]

    def phase_b2(i, _):
        for n in range(3):
            for pair in range(2):
                pl.when(i == 4 * n + pair)(lambda n=n, pair=pair: sends[n][pair]().start())
        sweep(2 - lax.div(i, 4), lax.rem(i, 4))
        return 0

    for p in range(2):
        w.got_partner(p)
        for c in range(2):
            build(p, c, range(4))
    lax.fori_loop(0, 8, phase_0, 0)
    lax.fori_loop(0, 14, phase_a4, 0)
    lax.fori_loop(0, 4, phase_b1, 0)
    lax.fori_loop(0, 12, phase_b2, 0)
    for pairs in sends:
        for cp in pairs:
            cp().wait()
    for wait in w.sent:
        wait()
    for t in range(4):
        out_ref[t] = (yt[0, t] + yin[0, t] + yin[1, t] + yin[2, t]) * sign


def solution(mesh):
    grid = Mesh(mesh.devices.reshape(2, 4, 4, 4), ('c', 'z', 'y', 'x'))
    spec = P(('z', 'y', 'x', 'c'), None)

    def per_device(x, v, ell, scale):
        anym, smem = pl.BlockSpec(memory_space=pl.ANY), pl.BlockSpec(memory_space=pltpu.SMEM)
        yt = pl.pallas_call(
            kernel,
            out_shape=jax.ShapeDtypeStruct((4, 128, TILE), F32),
            name='comm',
            in_specs=[smem, smem, anym, anym],
            out_specs=pl.BlockSpec(memory_space=pltpu.VMEM),
            scratch_shapes=[
                pltpu.VMEM((NPOS, 2, ROWS, 128), BF16),
                pltpu.VMEM((NPOS, 2, HALF, 128), BF16),
                pltpu.VMEM((4, 4, 2, TILE, 128), BF16),
                pltpu.VMEM((4, 4, 128, TILE), F32),
                pltpu.VMEM((3, 4, 128, TILE), F32),
                pltpu.VMEM((BLK, 128), BF16),
                pltpu.SemaphoreType.DMA((3,)),
                pltpu.SemaphoreType.DMA((100,)),
                pltpu.SemaphoreType.DMA((NPOS, 2)),
                pltpu.SemaphoreType.DMA((NPOS,)),
                pltpu.SemaphoreType.DMA((6,)),
                pltpu.SemaphoreType.DMA((2, 3, 2)),
            ],
            compiler_params=pltpu.CompilerParams(vmem_limit_bytes=60 * 2 ** 20, collective_id=0, has_side_effects=True),
        )(ell, scale, x, v)
        return yt.transpose(0, 2, 1).reshape(BLK, 128)

    return jax.shard_map(per_device, mesh=grid, in_specs=(spec, spec, P(None), P(None)), out_specs=spec, check_vma=False)
```

```python
import functools

import jax
import jax.numpy as jnp
from jax import lax
from jax.experimental import pallas as pl
from jax.experimental.pallas import tpu as pltpu
from jax.sharding import Mesh, PartitionSpec as P

F32 = jnp.float32
BF16 = jnp.bfloat16
MESH = pl.DeviceIdType.MESH
BLK = 1024
TILE = 256
HALF = 512
AUG0 = 2 * HALF
ROWS = AUG0 + 4 * 8
XROWS = 144
BF16_MAX = 3.3895313892515355e38

A, B = 0, 1
ORDER = [(0, 0, A), (0, 0, B),
         (0, -1, A), (0, 1, A), (-1, 0, B), (1, 0, B),
         (0, -1, B), (0, 1, B), (-1, 0, A), (1, 0, A),
         (-1, -1, B), (-1, 1, B), (-1, -1, A), (1, -1, A),
         (1, -1, B), (1, 1, B), (-1, 1, A), (1, 1, A),
         (0, 2, A), (2, 0, B), (0, 2, B), (2, 0, A),
         (2, -1, B), (2, 1, B), (-1, 2, A), (1, 2, A),
         (-1, 2, B), (1, 2, B), (2, -1, A), (2, 1, A),
         (2, 2, B), (2, 2, A)]
POS = {key: i for i, key in enumerate(ORDER)}
NPOS = len(ORDER)


def wrap(d):
    return (d + 1) % 4 - 1


def split3(n):
    hi = jnp.minimum(n, BF16_MAX).astype(BF16).astype(F32)
    r = n - hi
    mid = r.astype(BF16).astype(F32)
    return hi, mid, r - mid


class Wires:
    def __init__(self, cols, send, ici, d2d, pos):
        self.cols, self.send, self.ici, self.d2d, self.pos = cols, send, ici, d2d, pos
        self.sent = []
        self.dev = {(a, d): {a: lax.rem(pos[a] + d + 4, 4)} for a in 'zyx' for d in (1, -1, 2)}
        self.mate = {'c': 1 - pos['c']}

    def _copy(self, src, dst, recv, dev):
        n = len(self.sent)
        self.sent.append(lambda: pltpu.make_async_copy(src(), src(), self.send.at[n]).wait())
        pltpu.make_async_remote_copy(src_ref=src(), dst_ref=dst(), send_sem=self.send.at[n], recv_sem=recv(),
                                     device_id=dev, device_id_type=MESH).start()

    def block(self, key, c=0, part=None):
        p = POS[key]
        if part is None:
            return lambda: self.cols.at[p, c]
        return lambda: self.cols.at[p, c, pl.ds(part * (ROWS // 2), ROWS // 2)]

    def sem(self, key, part=0):
        return lambda: self.ici.at[POS[key], part]

    def both(self, axis, key):
        for sign in (1, -1):
            dz, dy, h = key
            dst = (dz, wrap(dy - sign), h) if axis == 'y' else (wrap(dz - sign), dy, h)
            self._copy(self.block(key), self.block(dst), self.sem(dst), self.dev[axis, sign])

    def relay(self, axis, off, h):
        dst = (off, 2, h) if axis == 'y' else (2, off, h)
        for part, sign in ((0, 1), (1, -1)):
            src = (off, -sign, h) if axis == 'y' else (-sign, off, h)
            self._copy(self.block(src, 0, part), self.block(dst, 0, part), self.sem(dst, part), self.dev[axis, sign])

    def partner(self, key):
        self._copy(self.block(key, 0), self.block(key, 1), lambda: self.d2d.at[POS[key]], self.mate)

    def _recv(self, dst, sem):
        pltpu.make_async_copy(dst, dst, sem).wait()

    def got(self, key):
        for part in (0, 1) if self.halved(key) else (None,):
            self._recv(self.block(key, 0, part)(), self.sem(key, part or 0)())

    @staticmethod
    def halved(key):
        dz, dy, h = key
        last = (dz if dz != 0 else dy) if h == A else (dy if dy != 0 else dz)
        return last == 2

    def got_partner(self, p):
        self._recv(self.cols.at[p, 1], self.d2d.at[p])


def schedule(w):
    def slot1():
        for key in [(0, -1, A), (0, 1, A), (-1, 0, B), (1, 0, B)]:
            w.got(key)
            w.partner(key)
        for d in (-1, 1):
            w.both('y', (d, 0, B))
            w.both('z', (0, d, A))
        w.relay('y', 0, A)
        w.relay('z', 0, B)

    def slot2():
        for key in [(0, -1, B), (0, 1, B), (-1, 0, A), (1, 0, A)]:
            w.got(key)
            w.partner(key)
        w.relay('y', 0, B)
        w.relay('z', 0, A)

    def slot3():
        for key in [(-1, -1, B), (-1, 1, B), (-1, -1, A), (1, -1, A)]:
            w.got(key)
            w.partner(key)

    def slot4():
        for key in [(0, 2, A), (2, 0, B)]:
            w.got(key)
            w.partner(key)
        w.both('y', (2, 0, B))
        w.both('z', (0, 2, A))
        for key in [(1, -1, B), (1, 1, B), (-1, 1, A), (1, 1, A)]:
            w.got(key)
            w.partner(key)
        for d in (-1, 1):
            w.relay('y', d, B)
            w.relay('z', d, A)

    def slot5():
        for key in [(0, 2, B), (2, 0, A)]:
            w.got(key)
            w.partner(key)

    def slot6():
        for key in [(2, -1, B), (2, 1, B), (-1, 2, A), (1, 2, A)]:
            w.got(key)
            w.partner(key)
        w.relay('y', 2, B)
        w.relay('z', 2, A)

    def slot7():
        for key in [(-1, 2, B), (1, 2, B), (2, -1, A), (2, 1, A)]:
            w.got(key)
            w.partner(key)

    def slot8():
        for key in [(2, 2, B), (2, 2, A)]:
            w.got(key)
            w.partner(key)

    return {1: slot1, 4: slot2, 8: slot3, 9: slot4, 10: slot5, 12: slot6, 14: slot7, 15: slot8}


def kernel(ell_ref, scale_ref, x_ref, v_ref, out_ref, cols, ag, xr, yt, yin, vbuf, local, send, ici, d2d, xsem, ysem):
    pos = {k: lax.axis_index(k) for k in ('c', 'z', 'y', 'x')}
    w = Wires(cols, send, ici, d2d, pos)
    xdev = lambda d: w.dev['x', d]

    loads = [pltpu.make_async_copy(x_ref.at[pl.ds(h * HALF, HALF)], cols.at[h, 0, pl.ds(0, HALF)], local.at[h]) for h in range(2)]
    loads.append(pltpu.make_async_copy(v_ref, vbuf, local.at[2]))
    for cp in loads:
        cp.start()
    barrier = pltpu.get_barrier_semaphore()
    peers = [w.dev[a, d] for a in 'zy' for d in (1, -1)] + [xdev(1), xdev(-1), xdev(2), w.mate]
    for dev in peers:
        pl.semaphore_signal(barrier, inc=1, device_id=dev, device_id_type=MESH)
    xr[:, :, :, pl.ds(XROWS, TILE - XROWS), :] = jnp.zeros((4, 4, 2, TILE - XROWS, 128), BF16)
    yt[...] = jnp.zeros_like(yt)

    ell = jnp.full((8, 128), ell_ref[0], F32)
    size = jnp.abs(jnp.full((8, 128), scale_ref[0], F32))
    two_ell_sq = 2.0 * ell * ell
    unit = jnp.exp2(jnp.clip(-jnp.ceil(jnp.log2(two_ell_sq)), -126.0, 40.0)).astype(BF16).astype(F32)
    unit = jnp.where(two_ell_sq > 3.4028234e38, 0.0, unit)
    factor = jnp.where(unit > 0.0, -1.4426950408889634 / (unit * two_ell_sq), -1.0)
    shift = jnp.maximum(jnp.log2(size), -400.0) / factor
    negc, cap = factor[0, 0], size[0, 0]
    sign = jnp.where(jnp.full((8, 128), scale_ref[0], F32) < 0.0, -1.0, 1.0)[0, 0]
    unit, shift = unit[:1], shift[:1]

    for cp in loads:
        cp.wait()
    for t in range(8):
        half, at = t // 4, (t % 4) * 128
        xt = cols[half, 0, pl.ds(at, 128), :].astype(F32).T
        norm = jnp.sum(xt * xt, axis=0, keepdims=True)
        hi, mid, lo = split3(norm)
        row = lax.broadcasted_iota(jnp.int32, (16, 128), 0)
        ones = jnp.where(row < 6, 1.0, 0.0)
        left = jnp.where(row == 0, hi, jnp.where(row == 1, mid, jnp.where(row == 2, lo, ones)))
        hi, mid, lo = split3(norm * unit + shift)
        right = jnp.where(row == 3, hi, jnp.where(row == 4, mid, jnp.where(row == 5, lo, ones * unit)))
        cols[half, 0, pl.ds(AUG0 + (t % 4) * 8, 8), :] = left[:8].astype(BF16)
        xr[0, t // 2, t % 2, pl.ds(0, 128), :] = (xt * (-2.0 * unit)).astype(BF16)
        xr[0, t // 2, t % 2, pl.ds(128, 16), :] = right.astype(BF16)
        cols[half, 0, pl.ds(HALF + at, 128), :] = vbuf[pl.ds(t * 128, 128), :].astype(F32).T.astype(BF16)
    pl.semaphore_wait(barrier, len(peers))

    def xcopy(src, dst, tiles, recv, d):
        cut = lambda b: lambda: xr.at[b, pl.ds(*tiles), :, pl.ds(0, XROWS)]
        w._copy(cut(src), cut(dst), lambda: xsem.at[recv], xdev(d))

    def xgot(dst, tiles, recv):
        ref = xr.at[dst, pl.ds(*tiles), :, pl.ds(0, XROWS)]
        pltpu.make_async_copy(ref, ref, xsem.at[recv]).wait()

    w.partner((0, 0, A))
    w.partner((0, 0, B))
    for part in range(2):
        xcopy(0, 1, (2 * part, 2), part, 1)
        xcopy(0, 2, (2 * part, 2), 2 + part, -1)
    w.both('y', (0, 0, A))
    w.both('z', (0, 0, B))
    w.both('y', (0, 0, B))
    w.both('z', (0, 0, A))

    def build(p, c, tiles):
        for lt in tiles:
            piece = cols[p, c, pl.ds(AUG0 + lt * 8, 8), :].astype(F32)
            full = jnp.concatenate([piece, jnp.zeros((120, 128), F32)], axis=0)
            ag[p, c, pl.ds(lt * 128, 128), :] = full.T.astype(BF16)

    def gram(p, xb, pair, cores):
        lhs = jnp.concatenate([jnp.concatenate([cols[p, c, pl.ds(0, HALF), :], ag[p, c]], axis=1) for c in cores], axis=0)
        rhs = jnp.concatenate([jnp.concatenate([xr[xb, pair * 2 + q, h] for h in range(2)], axis=1) for q in range(2)], axis=1)
        return jnp.dot(lhs, rhs, preferred_element_type=F32)

    def values(dist):
        kern = jnp.exp2(dist * negc).astype(BF16)
        return jnp.minimum(kern, jnp.full(kern.shape, cap, F32).astype(BF16))

    def product(p, xb, pair, cores, kern):
        vt = jnp.concatenate([cols[p, c, pl.ds(HALF + 128 * k, 128), :] for c in cores for k in range(4)], axis=1)
        r = jnp.dot(vt, kern, preferred_element_type=F32)
        for q in range(2):
            yt[xb, pair * 2 + q] += r[:, q * TILE:(q + 1) * TILE]

    def group(work):
        todo = [(p, xb, pair, cores) for ps, xb, pair in work for p in ps for cores in ((0,), (1,))]
        dist = gram(*todo[0])
        for n, (p, xb, pair, cores) in enumerate(todo):
            now = dist
            if n + 1 < len(todo):
                dist = gram(*todo[n + 1])
            product(p, xb, pair, cores, values(now))

    acts = schedule(w)

    def phase_0(k, _):
        @pl.when(k == 2)
        def _():
            xgot(1, (0, 2), 0)

        @pl.when(k == 3)
        def _():
            xgot(2, (0, 2), 2)
            xcopy(1, 3, (0, 2), 4, 1)

        @pl.when(k == 4)
        def _():
            xgot(1, (2, 2), 1)

        @pl.when(k == 5)
        def _():
            xgot(2, (2, 2), 3)
            xcopy(2, 3, (2, 2), 5, -1)
            acts[1]()

        @pl.when(k == 6)
        def _():
            xgot(3, (0, 2), 4)

        @pl.when(k == 7)
        def _():
            xgot(3, (2, 2), 5)
            w.got_partner(2)

        a, b = lax.div(k, 2), lax.rem(k, 2)
        e = lax.div(a + 1, 2)
        inner = lax.rem(e, 2)
        xb = inner * (1 + b) + (1 - inner) * 3 * lax.div(e, 2)
        pair = inner * (a - 1) + (1 - inner) * b
        group([((0, 1), xb, pair)])
        for c in range(2):
            build(1 + lax.div(k, 7), c, range(4))
        return 0

    def phase_a4(n, _):
        p = n + 2
        for at, act in acts.items():
            if at > 1:
                pl.when(p == at)(act)
        w.got_partner(p + 1)
        late = p + lax.div(p, 12) * (5 - 3 * lax.div(p, 15))
        pl.when((p >= 12) & (p < 15))(lambda: w.got_partner(p + 5))
        group([((p,), xb, pair) for xb in range(4) for pair in range(2)])
        for c in range(2):
            build(p + 1, c, range(4))
            build(late, c, range(4))
        return 0

    def sweep(xb, i):
        p = 16 + 4 * i
        group([([p + k for k in range(4)], xb, pair) for pair in range(2)])

    def phase_b1(i, _):
        @pl.when(i < 3)
        def _():
            for k in range(4):
                w.got_partner(20 + 4 * i + k)

        sweep(3, i)
        for k in range(4):
            for c in range(2):
                build(16 + lax.rem(4 * i + 4 + k, 16), c, range(4))
        return 0

    def ysend(label, d, slot, pair):
        tiles = pl.ds(2 * pair, 2)
        return lambda: pltpu.make_async_remote_copy(
            src_ref=yt.at[label, tiles], dst_ref=yin.at[slot, tiles], send_sem=ysem.at[0, slot, pair],
            recv_sem=ysem.at[1, slot, pair], device_id=xdev(d), device_id_type=MESH)

    sends = [[ysend(*who, pair) for pair in range(2)] for who in ((3, 2, 2), (2, 1, 0), (1, -1, 1))]

    def phase_b2(i, _):
        for n in range(3):
            for pair in range(2):
                pl.when(i == 2 * n + pair)(lambda n=n, pair=pair: sends[n][pair]().start())
        p = 16 + 8 * lax.rem(i, 2)
        group([([p + k for k in range(8)], 2 - lax.div(i, 2), pair) for pair in range(2)])
        return 0

    for p in range(2):
        w.got_partner(p)
        for c in range(2):
            build(p, c, range(4))
    lax.fori_loop(0, 8, phase_0, 0)
    lax.fori_loop(0, 14, phase_a4, 0)
    lax.fori_loop(0, 4, phase_b1, 0)
    lax.fori_loop(0, 6, phase_b2, 0)
    for pairs in sends:
        for cp in pairs:
            cp().wait()
    for wait in w.sent:
        wait()
    for t in range(4):
        out_ref[t] = (yt[0, t] + yin[0, t] + yin[1, t] + yin[2, t]) * sign


def solution(mesh):
    grid = Mesh(mesh.devices.reshape(2, 4, 4, 4), ('c', 'z', 'y', 'x'))
    spec = P(('z', 'y', 'x', 'c'), None)

    def per_device(x, v, ell, scale):
        anym, smem = pl.BlockSpec(memory_space=pl.ANY), pl.BlockSpec(memory_space=pltpu.SMEM)
        yt = pl.pallas_call(
            kernel,
            out_shape=jax.ShapeDtypeStruct((4, 128, TILE), F32),
            name='comm',
            in_specs=[smem, smem, anym, anym],
            out_specs=pl.BlockSpec(memory_space=pltpu.VMEM),
            scratch_shapes=[
                pltpu.VMEM((NPOS, 2, ROWS, 128), BF16),
                pltpu.VMEM((NPOS, 2, HALF, 128), BF16),
                pltpu.VMEM((4, 4, 2, TILE, 128), BF16),
                pltpu.VMEM((4, 4, 128, TILE), F32),
                pltpu.VMEM((3, 4, 128, TILE), F32),
                pltpu.VMEM((BLK, 128), BF16),
                pltpu.SemaphoreType.DMA((3,)),
                pltpu.SemaphoreType.DMA((100,)),
                pltpu.SemaphoreType.DMA((NPOS, 2)),
                pltpu.SemaphoreType.DMA((NPOS,)),
                pltpu.SemaphoreType.DMA((6,)),
                pltpu.SemaphoreType.DMA((2, 3, 2)),
            ],
            compiler_params=pltpu.CompilerParams(vmem_limit_bytes=60 * 2 ** 20, collective_id=0, has_side_effects=True),
        )(ell, scale, x, v)
        return yt.transpose(0, 2, 1).reshape(BLK, 128)

    return jax.shard_map(per_device, mesh=grid, in_specs=(spec, spec, P(None), P(None)), out_specs=spec, check_vma=False)
```
